32 devices in a mesh: row: 2 (over x), col: 4 (over z), chan: 4 (over y, core).
Axes of the slice: x: 2, y: 2, z: 4, core: 2. Of those that a mesh axis runs over, the one named last changes fastest.
Arguments:
- image_gen: float32 [3, 512, 4096], P(None, ('row', 'chan'), 'col'), may hold values from -3 to 3
- image_ref: float32 [3, 512, 4096], P(None, ('row', 'chan'), 'col'), may hold values from -1 to 1
- kernel_one: bfloat16 [3, 3, 48, 64], replicated, may hold values from -0.3125 to 0.3125
- bias_one: float32 [64], replicated, may hold values from -1.5 to 1.5
- kernel_two: bfloat16 [5, 5, 64, 192], replicated, may hold values from -0.15625 to 0.15625
- bias_two: float32 [192], replicated, may hold values from -1.5 to 1.5
- kernel_three: bfloat16 [3, 3, 192, 384], P(None, None, None, 'chan'), may hold values from -0.15625 to 0.15625
- bias_three: float32 [384], replicated, may hold values from -1.5 to 1.5
- lin_first: float32 [64], replicated, may hold values from 0.1 to 1
- lin_second: float32 [192], replicated, may hold values from 0.1 to 1
- lin_third: float32 [384], replicated, may hold values from 0.1 to 1
Outputs:
- image_grad: float32 [3, 512, 4096], P(None, ('row', 'chan'), 'col')
- loss: float32 [], replicated
The draws below stay inside these ranges and needn't reach their ends.
All inputs are finite; a program needn't handle non-finite values.
Results may differ from the reference program's by a relative error of at most 0.0086.
Values may be sent and summed in bfloat16 or wider, within the bound.
No kernel may reach another device: no remote copies, remote signals or barrier semaphores. Data moves between devices by JAX's collectives and lax.ppermute only.
A program may use at most 128 MiB of HBM per device.

```python
import math
import jax
import jax.numpy as jnp
from jax import lax

CH1 = 64
CH2 = 192
CH3 = 384
HEIGHT = 512
WIDTH = 4096


def frame_pair(key):
    base = jax.random.fold_in(key, 7101)
    first_key, second_key = jax.random.split(base)
    shape = (3, HEIGHT, WIDTH)
    reference_frame = jax.random.uniform(first_key, shape, jnp.float32, -1.0, 1.0)
    noise = jax.random.normal(second_key, shape, jnp.float32)
    lowest = 0.25
    highest = 0.75
    position = jnp.arange(HEIGHT).astype(jnp.float32) / HEIGHT
    amplitude = lowest + (highest - lowest) * position
    generated = jnp.clip(reference_frame + amplitude[None, :, None] * noise, -3.0, 3.0)
    return (generated, reference_frame)


def draw_image_gen(key, part):
    return frame_pair(key)[0]


def draw_image_ref(key, part):
    return frame_pair(key)[1]


def shard_levels(rng, shape, cuts, least, top_value):
    loudness = 1.0
    for dim, shards_of in cuts:
        heights = jax.random.uniform(jax.random.fold_in(jax.random.fold_in(rng, 6), dim), (shards_of,), jnp.float32, least / len(cuts), top_value / len(cuts))
        loudness = loudness * jnp.repeat(jnp.exp(heights), shape[dim] // shards_of).reshape((-1,) + (1,) * (len(shape) - 1 - dim))
    return loudness


def scatter_about(rng, extent, width, reach, cuts=(), kind=jnp.bfloat16):
    values = jax.random.normal(rng, extent, jnp.float32) * width
    if len(cuts) > 0:
        values = shard_levels(rng, extent, cuts, -0.22, 0.18) * values
    return jnp.clip(values, min=-reach, max=reach).astype(kind)


def setup_inputs(seed: int = 0) -> dict:
    streams_of = jax.random.split(jax.random.key(seed), 12)
    image_gen = draw_image_gen(jax.random.fold_in(streams_of[11], 71), 0)
    image_ref = draw_image_ref(jax.random.fold_in(streams_of[11], 71), 0)
    kernel_one = scatter_about(streams_of[2], (3, 3, 48, CH1), 432 ** -0.5, 0.3125)
    bias_one = scatter_about(streams_of[3], (CH1,), 0.3, 1.5, (), jnp.float32)
    kernel_two = scatter_about(streams_of[4], (5, 5, CH1, CH2), (25 * CH1) ** -0.5, 0.15625)
    bias_two = scatter_about(streams_of[5], (CH2,), 0.3, 1.5, (), jnp.float32)
    kernel_three = scatter_about(streams_of[6], (3, 3, CH2, CH3), (9 * CH2) ** -0.5, 0.15625, ((3, 4),))
    bias_three = scatter_about(streams_of[7], (CH3,), 0.3, 1.5, (), jnp.float32)
    lin_first = jnp.clip(jnp.exp(jax.random.uniform(streams_of[8], (CH1,), jnp.float32, math.log(0.1), math.log(1.0))), 0.1, 1.0)
    lin_second = jnp.clip(jnp.exp(jax.random.uniform(streams_of[9], (CH2,), jnp.float32, math.log(0.1), math.log(1.0))), 0.1, 1.0)
    lin_third = jnp.clip(jnp.exp(jax.random.uniform(streams_of[10], (CH3,), jnp.float32, math.log(0.1), math.log(1.0))), 0.1, 1.0)
    return {"image_gen": image_gen, "image_ref": image_ref, "kernel_one": kernel_one, "bias_one": bias_one, "kernel_two": kernel_two, "bias_two": bias_two, "kernel_three": kernel_three, "bias_three": bias_three, "lin_first": lin_first, "lin_second": lin_second, "lin_third": lin_third}


OFFSETS = (-0.03, -0.088, -0.188)
SPREADS = (0.458, 0.448, 0.45)
EPSILON = 1e-06

def normed_cells(image):
    offsets = jnp.array(OFFSETS, jnp.float32)[:, None, None]
    spreads = jnp.array(SPREADS, jnp.float32)[:, None, None]
    scaled = ((image - offsets) / spreads).astype(jnp.bfloat16)
    planes, height, columns = image.shape
    blocks = scaled.reshape(planes, height // 4, 4, columns // 4, 4)
    return blocks.transpose(0, 2, 4, 1, 3).reshape(planes * 16, height // 4, columns // 4)

def from_cells(values):
    planes, height, columns = values.shape
    blocks = values.reshape(planes // 16, 4, 4, height, columns)
    return blocks.transpose(0, 3, 1, 4, 2).reshape(planes // 16, height * 4, columns * 4)

def conv_valid(padded, kernel):
    return lax.conv_general_dilated(padded, kernel, (1, 1), 'VALID', dimension_numbers=('NCHW', 'HWIO', 'NCHW'), preferred_element_type=jnp.float32)

def padded_by(values, margin):
    return jnp.pad(values, ((0, 0), (0, 0), (margin, margin), (margin, margin)))

def flipped(kernel):
    return jnp.swapaxes(kernel[::-1, ::-1], 2, 3)

def pooled(values):
    batch, planes, height, columns = values.shape
    return values.reshape(batch, planes, height // 2, 2, columns // 2, 2).mean(axis=(3, 5))

def unpooled(values):
    return 0.25 * jnp.repeat(jnp.repeat(values, 2, axis=-2), 2, axis=-1)

def activate(pre):
    return pre * jax.nn.sigmoid(pre)

def activate_slope(pre):
    sigma = jax.nn.sigmoid(pre)
    return sigma * (1.0 + pre * (1.0 - sigma))

def unit_terms(features, sums):
    scales = lax.rsqrt(sums + EPSILON)
    return (features * scales[:, None], scales)

def layer_loss(unit_vec, weights):
    differ = unit_vec[0] - unit_vec[1]
    return jnp.sum(weights[:, None, None] * differ * differ)

def slopes(unit_vec, features, weights, factor):
    slope = 2.0 * factor * weights[:, None, None] * (unit_vec[0] - unit_vec[1])
    return (slope, lax.optimization_barrier(jnp.sum(features[0] * slope, axis=0)))

def finish_grad(slope, features, scales, inners):
    first = scales[0]
    return first[None] * slope - features[0] * (first * first * first * inners)[None]

def reference(image_gen, image_ref, kernel_one, bias_one, kernel_two, bias_two, kernel_three, bias_three, lin_first, lin_second, lin_third):
    pixels = image_gen.shape[1] * image_gen.shape[2]
    stacked = jnp.stack([normed_cells(image_gen), normed_cells(image_ref)])
    pre_one = conv_valid(padded_by(stacked, 1), kernel_one) + bias_one[None, :, None, None]
    features_one = activate(pre_one)
    pool_one = pooled(features_one).astype(jnp.bfloat16)
    pre_two = conv_valid(padded_by(pool_one, 2), kernel_two) + bias_two[None, :, None, None]
    features_two = activate(pre_two)
    pool_two = pooled(features_two).astype(jnp.bfloat16)
    pre_three = conv_valid(padded_by(pool_two, 1), kernel_three) + bias_three[None, :, None, None]
    features_three = activate(pre_three)
    unit_one, scales_one = unit_terms(features_one, lax.optimization_barrier(jnp.sum(features_one * features_one, axis=1)))
    unit_two, scales_two = unit_terms(features_two, lax.optimization_barrier(jnp.sum(features_two * features_two, axis=1)))
    unit_three, scales_three = unit_terms(features_three, lax.optimization_barrier(jnp.sum(features_three * features_three, axis=1)))
    count_one = pixels // 16
    count_two = pixels // 64
    count_three = pixels // 256
    loss = layer_loss(unit_one, lin_first) / count_one + layer_loss(unit_two, lin_second) / count_two + layer_loss(unit_three, lin_third) / count_three
    slope_one, inners_one = slopes(unit_one, features_one, lin_first, 16.0)
    slope_two, inners_two = slopes(unit_two, features_two, lin_second, 64.0)
    slope_three, inners_three = slopes(unit_three, features_three, lin_third, 256.0)
    dfeat_three = finish_grad(slope_three, features_three, scales_three, inners_three)
    dpre_three = (dfeat_three * activate_slope(pre_three[0])).astype(jnp.bfloat16)
    dpool_two = conv_valid(padded_by(dpre_three[None], 1), flipped(kernel_three))[0]
    dfeat_two = finish_grad(slope_two, features_two, scales_two, inners_two) + unpooled(dpool_two)
    dpre_two = (dfeat_two * activate_slope(pre_two[0])).astype(jnp.bfloat16)
    dpool_one = conv_valid(padded_by(dpre_two[None], 2), flipped(kernel_two))[0]
    dfeat_one = finish_grad(slope_one, features_one, scales_one, inners_one) + unpooled(dpool_one)
    dpre_one = (dfeat_one * activate_slope(pre_one[0])).astype(jnp.bfloat16)
    back_cells = conv_valid(padded_by(dpre_one[None], 1), flipped(kernel_one))[0]
    spreads = jnp.array(SPREADS, jnp.float32)[:, None, None]
    image_grad = from_cells(back_cells) / spreads
    return (image_grad, loss)
```

```python
import functools

import jax
import jax.numpy as jnp
import numpy as np
from jax import lax
from jax.experimental import pallas as pl
from jax.experimental.pallas import tpu as pltpu
from jax.sharding import PartitionSpec as P

OFFSETS = (-0.03, -0.088, -0.188)
SPREADS = (0.458, 0.448, 0.45)
EPSILON = 1e-06

S = 16
HJ = 6
RIM = 12
F32 = jnp.float32
BF16 = jnp.bfloat16
ROWS = ("row", "chan")
GUARD = 128


def up128(n):
    return -(-n // 128) * 128


def wide(column, lanes):
    return jnp.concatenate([column] * (lanes // 128), axis=1)


def column(row, times=1):
    n = row.shape[1]
    here = lax.broadcasted_iota(jnp.int32, (n, n), 0) == lax.broadcasted_iota(jnp.int32, (n, n), 1)
    one = jnp.sum(jnp.where(here, jnp.broadcast_to(row[...], (n, n)), 0.0), axis=1, keepdims=True)
    one = jnp.broadcast_to(one, (n, 128))
    return jnp.concatenate([one] * times, axis=0) if times > 1 else one


def sigmoid(v):
    return 0.5 + 0.5 * jnp.tanh(0.5 * v)


def lanes_of(values, start, count, total):
    part = values[:, start : start + count]
    if total == count:
        return part
    return jnp.concatenate([part, jnp.zeros((values.shape[0], total - count), values.dtype)], axis=1)


def layer_terms(v0, v1, lin, factor):
    g0 = sigmoid(v0)
    f0 = v0 * g0
    f1 = v1 * sigmoid(v1)
    s0 = lax.rsqrt(jnp.sum(f0 * f0, axis=0, keepdims=True) + EPSILON)
    s1 = lax.rsqrt(jnp.sum(f1 * f1, axis=0, keepdims=True) + EPSILON)
    diff = f0 * s0 - f1 * s1
    weighted = lin * diff
    slope = (2.0 * factor) * weighted
    inner = jnp.sum(f0 * slope, axis=0, keepdims=True)
    dfeat = s0 * slope - f0 * (s0 * s0 * s0 * inner)
    return dfeat, g0 * (1.0 + v0 * (1.0 - g0)), jnp.sum(weighted * diff, axis=0, keepdims=True)


def shift_rows(dst, dst_row, dst_lane, src, src_row, count, start, width, chunk=64):
    def body(i, carry):
        a = pl.multiple_of(src_row + i * chunk, chunk)
        b = pl.multiple_of(dst_row + i * chunk, 16)
        part = src[pl.ds(a, chunk), :]
        dst[pl.ds(b, chunk), dst_lane : dst_lane + width] = part[:, start : start + width].astype(BF16)
        return carry

    lax.fori_loop(0, count // chunk, body, 0)


def weights_kernel(R, C, high, across, place, want, k1, k2, k3, w1, w1b, w2, w2b, k3t, masks, t1):
    taps = k1.shape[0]
    ch1 = k1.shape[1]
    pick = lax.broadcasted_iota(jnp.int32, (768, taps), 0) == want[...]
    t1[200:968, :] = jnp.dot(jnp.where(pick, 1.0, 0.0).astype(BF16), k1[...], preferred_element_type=F32)
    t1[0:200, :] = jnp.zeros((200, ch1), F32)
    t1[968:, :] = jnp.zeros((t1.shape[0] - 968, ch1), F32)
    for ci in range(2):
        for cj in range(2):
            moved = t1[200 - cj * 192 - ci * 4 : 968 - cj * 192 - ci * 4, :]
            row = (ci * 2 + cj) * ch1
            w1[row : row + ch1, :] = moved.T.astype(BF16)
    for wi in range(4):
        low = 200 - 4 * (wi % 2)
        half = 1 if wi < 2 else 0
        for wj in range(0, 4, 2):
            parts = []
            for e in range(2):
                start = low + (2 - wj - e) * 192
                block = t1[start : start + 384, :].reshape(24, 2, 8, ch1)[:, half]
                parts.append(block.reshape(192, ch1))
            lane = (wi * 4 + wj) * ch1
            w1b[:, lane : lane + 2 * ch1] = jnp.concatenate(parts, axis=1).astype(BF16)
    size = 5
    ch2 = k2.shape[3]
    none = jnp.zeros((ch1, ch2), F32)

    def tap(y, x):
        return k2[y, x].astype(F32) if 0 <= x < size else none

    for pi in range(2):
        w = 5 * (1 - pi)
        lane = (w // 2) * 12 + (w % 2) * 2
        for x in range(3):
            a = (lane + 4 * x) * ch1
            w2[pi * 2 * ch2 : (pi + 1) * 2 * ch2, a : a + 2 * ch1] = jnp.zeros((2 * ch2, 2 * ch1), BF16)
            a = (lane + 4 * x) * ch2
            w2b[pi * 2 * ch1 : (pi + 1) * 2 * ch1, a : a + 2 * ch2] = jnp.zeros((2 * ch1, 2 * ch2), BF16)
    for y in range(size):
        for pj in range(2):
            for x in range(3):
                pair = jnp.concatenate([tap(y, 2 * x - pj), tap(y, 2 * x + 1 - pj)], axis=0).T.astype(BF16)
                back = jnp.concatenate(
                    [tap(size - 1 - y, size - 1 - 2 * x + pj), tap(size - 1 - y, size - 2 - 2 * x + pj)], axis=1
                ).astype(BF16)
                for pi in range(2):
                    w = y + pi
                    lane = ((w // 2) * 3 + x) * 4 + (w % 2) * 2
                    row = (pi * 2 + pj) * ch2
                    w2[row : row + ch2, lane * ch1 : (lane + 2) * ch1] = pair
                    row = (pi * 2 + pj) * ch1
                    w2b[row : row + ch1, lane * ch2 : (lane + 2) * ch2] = back
    for k in range(0, 9, 2):
        n = min(2, 9 - k) * ch2
        k3t[:, k * ch2 : k * ch2 + n] = k3[k * ch2 : k * ch2 + n, :].astype(F32).T.astype(BF16)
    W = C + 2 * HJ
    lane = lax.broadcasted_iota(jnp.int32, (1, masks.shape[1]), 1)
    i = ((lane.astype(F32) + 0.5) * (1.0 / W)).astype(jnp.int32)
    j = lane - i * W - HJ
    frames = (
        (0, R, False), (0, R + 1, True), (-1, R + 1, True), (-3, R + 6, False), (-2, R + 4, False),
        (-1, R + 2, False), (-1, R + 2, True), (0, R, True), (0, R + 1, False), (-1, R + 1, False),
    )
    masks[...] = jnp.zeros(masks.shape, F32)
    for n, (start, count, mine) in enumerate(frames):
        r, c = i + start, j
        rows, columns = R, C
        if not mine:
            r, c = r + place[0] * R, c + place[1] * C
            rows, columns = R * high, C * across
        ok = (i < count) & (r >= 0) & (r < rows) & (c >= 0) & (c < columns)
        masks[n : n + 1, :] = jnp.where(ok, 1.0, 0.0)


def cells_kernel(R, C, par, img, w1, b1, masks, pre, pool, msg_a, msg_b, sel, z, p1):
    W = C + 2 * HJ
    G = W + 4
    frame = up128((R + 1) * W)
    px = W * S
    K = sel.shape[0]
    rows = R * S + 2 * RIM
    tile = 256
    for t in range(K // tile):
        p = lax.broadcasted_iota(jnp.int32, (K, tile), 0)
        n = lax.broadcasted_iota(jnp.int32, (K, tile), 1) + t * tile
        want = (p & (S - 1)) * G + (p >> 4)
        sel[:, t * tile : (t + 1) * tile] = jnp.where((n == want) & (p < px), 1.0, 0.0).astype(BF16)
    for f in range(2):
        for t in range(K // tile):
            z[f, :, t * tile : (t + 1) * tile] = jnp.dot(
                img[f], sel[:, t * tile : (t + 1) * tile], preferred_element_type=F32
            )
    own = masks[0:1, 0 : R * W]
    bias = wide(column(b1, 4), tile)
    for pi in range(2):
        top = 8 - 8 * pi
        for pj in range(2):
            for f in range(2):
                for s in range(S):
                    q = s + 8 * pj - 4
                    lane = (q % S) * G + q // S
                    parts = []
                    for k in range(R + 1):
                        r = top + S * k
                        parts.append(
                            jnp.concatenate(
                                [z[f, c * rows + r : c * rows + r + S, lane : lane + W] for c in range(3)], axis=0
                            )
                        )
                    parts.append(jnp.zeros((3 * S, frame - (R + 1) * W), F32))
                    p1[s * 48 : s * 48 + 48, f * frame : (f + 1) * frame] = jnp.concatenate(parts, axis=1).astype(BF16)
            for t in range(2 * frame // tile):
                lanes = slice(t * tile, (t + 1) * tile)
                pre[pi, pj, :, lanes] = jnp.dot(w1[...], p1[:, lanes], preferred_element_type=F32) + bias
            for f in range(2):
                v = pre[pi, pj, :, f * frame : (f + 1) * frame]
                feat = v * sigmoid(v)
                quarter = feat.shape[0] // 4
                mean = 0.25 * (
                    (feat[0:quarter] + feat[quarter : 2 * quarter])
                    + (feat[2 * quarter : 3 * quarter] + feat[3 * quarter :])
                )
                mine = mean[:, pi * W : pi * W + R * W]
                mine = jnp.where(own > 0.0, mine, 0.0)
                row = (f * 4 + pi * 2 + pj) * quarter
                even = lax.rem(par[0], 2) == 0
                head = lanes_of(mine, 0, 3 * W, msg_a.shape[1])
                tail = lanes_of(mine, (R - 3) * W, 3 * W, msg_a.shape[1])
                msg_a[row : row + quarter, :] = jnp.where(even, tail, head).astype(BF16)
                msg_b[row : row + quarter, :] = jnp.where(even, head, tail).astype(BF16)
                pool[row : row + quarter, :] = lanes_of(mine, 0, R * W, pool.shape[1]).astype(BF16)


def first_grad_kernel(R, C, pre, lin, masks, w3, base, gain, loss, w3b):
    frame = base.shape[3]
    ch = lin.shape[1]
    c3 = w3.shape[0]
    c2 = w3b.shape[0]
    for k in range(9):
        w3b[:, k * c3 : (k + 1) * c3] = w3[:, (8 - k) * c2 : (9 - k) * c2].astype(F32).T.astype(BF16)
    total = jnp.zeros((1, frame), F32)
    weights = wide(column(lin), frame)
    for pi in range(2):
        for pj in range(2):
            for t in range(4):
                v0 = pre[pi, pj, t * ch : (t + 1) * ch, 0:frame]
                v1 = pre[pi, pj, t * ch : (t + 1) * ch, frame : 2 * frame]
                dfeat, slope, part = layer_terms(v0, v1, weights, 16.0)
                base[pi, pj, t * ch : (t + 1) * ch, :] = dfeat * slope
                gain[pi, pj, t * ch : (t + 1) * ch, :] = 0.25 * slope
                total = total + jnp.where(masks[1 + pi : 2 + pi, 0:frame] > 0.0, part, 0.0)
    loss[...] = jnp.broadcast_to(total, loss.shape)


def middle_kernel(
    R, C, par, pool, rec_a, rec_b, masks, w2, b2, lin2, w3, b3, lin3, w3b, d2, msg_a, msg_b, loss2, loss3,
    s1, p2, pre2, q2, s2, p3, pre3, s3, p3b,
):
    W = C + 2 * HJ
    even = lax.rem(par[0], 2) == 0
    n2 = up128((R + 4) * W)
    n3 = up128((R + 2) * W)
    n4 = up128(R * W)
    c1 = pool.shape[0] // 2
    c2 = b2.shape[1]
    c3 = b3.shape[1]
    ext = s1.shape[1]
    inside = masks[3:4, 0 : (R + 6) * W]
    for r in range(0, 2 * c1, 64):
        a = rec_a[r : r + 64, :].astype(F32)
        b = rec_b[r : r + 64, :].astype(F32)
        above = jnp.where(even, b, a)[:, 0 : 3 * W]
        below = jnp.where(even, a, b)[:, 0 : 3 * W]
        mine = pool[r : r + 64, :].astype(F32)[:, 0 : R * W]
        whole = jnp.concatenate([above, mine, below], axis=1)
        whole = jnp.where(inside > 0.0, whole, 0.0)
        s1[r : r + 64, :] = jnp.concatenate(
            [jnp.zeros((64, GUARD), F32), whole, jnp.zeros((64, ext - GUARD - (R + 6) * W), F32)], axis=1
        )
    for k in range(9):
        off = GUARD + (k // 3) * W + k % 3 - 1
        for f in range(2):
            shift_rows(p2, k * c1, f * n2, s1, f * c1, c1, off, n2)
    tile = 256
    bias2 = column(b2, 4)
    bias3 = column(b3)
    lins3 = column(lin3)

    def second(t, carry):
        lanes = pl.ds(pl.multiple_of(t * tile, tile), tile)
        v = jnp.dot(w2[...], p2[:, lanes], preferred_element_type=F32) + wide(bias2, tile)
        pre2[:, lanes] = v
        feat = v * sigmoid(v)
        q2[:, lanes] = 0.25 * (
            (feat[0:c2] + feat[c2 : 2 * c2]) + (feat[2 * c2 : 3 * c2] + feat[3 * c2 :])
        )
        return carry

    lax.fori_loop(0, 2 * n2 // tile, second, 0)
    for f in range(2):
        good = jnp.where(masks[4:5, 0:n2] > 0.0, q2[:, f * n2 : (f + 1) * n2], 0.0)
        s2[f * c2 : (f + 1) * c2, 0:GUARD] = jnp.zeros((c2, GUARD), F32)
        s2[f * c2 : (f + 1) * c2, GUARD : GUARD + n2] = good
        s2[f * c2 : (f + 1) * c2, GUARD + n2 :] = jnp.zeros((c2, s2.shape[1] - GUARD - n2), F32)
    for k in range(9):
        off = GUARD + (k // 3) * W + k % 3 - 1
        for f in range(2):
            shift_rows(p3, k * c2, f * n3, s2, f * c2, c2, off, n3)

    def third(t, carry):
        lanes = pl.ds(pl.multiple_of(t * tile, tile), tile)
        pre3[:, lanes] = jnp.dot(w3[...], p3[:, lanes], preferred_element_type=F32) + wide(bias3, tile)
        return carry

    lax.fori_loop(0, 2 * n3 // tile, third, 0)
    s3[:, 0:GUARD] = jnp.zeros((c3, GUARD), F32)
    s3[:, GUARD + n3 :] = jnp.zeros((c3, s3.shape[1] - GUARD - n3), F32)
    total = jnp.zeros((1, 128), F32)
    for t in range(n3 // 128):
        v0 = pre3[:, t * 128 : (t + 1) * 128]
        v1 = pre3[:, n3 + t * 128 : n3 + (t + 1) * 128]
        dfeat, slope, part = layer_terms(v0, v1, lins3, 256.0)
        lanes = slice(t * 128, (t + 1) * 128)
        s3[:, GUARD + t * 128 : GUARD + (t + 1) * 128] = jnp.where(masks[5:6, lanes] > 0.0, dfeat * slope, 0.0)
        total = total + jnp.where(masks[6:7, lanes] > 0.0, part, 0.0)
    loss3[...] = jnp.broadcast_to(total, loss3.shape)
    for k in range(9):
        off = GUARD + (k // 3) * W + k % 3 - 1
        shift_rows(p3b, k * c3, 0, s3, 0, c3, off, n4)
    up = 0.25 * jnp.dot(w3b[...], p3b[...], preferred_element_type=F32)
    total2 = jnp.zeros((1, n4), F32)
    weights = wide(column(lin2), n4)
    for t in range(4):
        rows = slice(t * c2, (t + 1) * c2)
        v0 = pre2[rows, 0:n2][:, 2 * W : 2 * W + n4]
        v1 = pre2[rows, n2 : 2 * n2][:, 2 * W : 2 * W + n4]
        dfeat, slope, part = layer_terms(v0, v1, weights, 64.0)
        d = jnp.where(masks[0:1, 0:n4] > 0.0, (dfeat + up) * slope, 0.0)
        d2[rows, :] = d.astype(BF16)
        total2 = total2 + jnp.where(masks[7:8, 0:n4] > 0.0, part, 0.0)
        head = lanes_of(d, 0, 2 * W, msg_a.shape[1])
        tail = lanes_of(d, (R - 2) * W, 2 * W, msg_a.shape[1])
        msg_a[rows, :] = jnp.where(even, tail, head).astype(BF16)
        msg_b[rows, :] = jnp.where(even, head, tail).astype(BF16)
    loss2[...] = jnp.broadcast_to(total2, loss2.shape)


def last_kernel(
    R, C, par, d2, rec_a, rec_b, masks, w2b, base, gain, w1b, out, s4, p2b, s5, p1b, g, sel, flat
):
    W = C + 2 * HJ
    even = lax.rem(par[0], 2) == 0
    c2 = d2.shape[0]
    frame = base.shape[3]
    n4 = up128(R * W)
    ext = s4.shape[1]
    ch = w2b.shape[0] // 4
    inside = masks[4:5, 0 : (R + 4) * W]

    def join(i, carry):
        rows = pl.ds(pl.multiple_of(i * 64, 64), 64)
        a = rec_a[rows, :].astype(F32)
        b = rec_b[rows, :].astype(F32)
        above = jnp.where(even, b, a)[:, 0 : 2 * W]
        below = jnp.where(even, a, b)[:, 0 : 2 * W]
        mine = d2[rows, :].astype(F32)[:, 0 : R * W]
        whole = jnp.concatenate([above, mine, below], axis=1)
        whole = jnp.where(inside > 0.0, whole, 0.0)
        s4[rows, :] = jnp.concatenate(
            [jnp.zeros((64, GUARD), F32), whole, jnp.zeros((64, ext - GUARD - (R + 4) * W), F32)], axis=1
        )
        return carry

    lax.fori_loop(0, c2 // 64, join, 0)
    for qi in range(2):
        for k in range(9):
            off = GUARD + (k // 3 + 1 - qi) * W + k % 3 - 1
            shift_rows(p2b, k * c2, 0, s4, 0, c2, off, frame)
        up = jnp.dot(w2b[qi * 2 * ch : (qi + 1) * 2 * ch, :], p2b[...], preferred_element_type=F32)
        good = masks[8 + qi : 9 + qi, 0:frame] > 0.0
        for qj in range(2):
            part = up[qj * ch : (qj + 1) * ch]
            for t in range(4):
                rows = slice(t * ch, (t + 1) * ch)
                d = base[qi, qj, rows, :] + gain[qi, qj, rows, :] * part
                row = ((qi * 2 + qj) * 4 + t) * ch
                s5[row : row + ch, 0:GUARD] = jnp.zeros((ch, GUARD), F32)
                s5[row : row + ch, GUARD : GUARD + frame] = jnp.where(good, d, 0.0)
                s5[row : row + ch, GUARD + frame :] = jnp.zeros((ch, s5.shape[1] - GUARD - frame), F32)
    for qi in range(2):
        for qj in range(2):
            for wi in range(4):
                for wj in range(4):
                    y, x = 2 * qi + wi - 1, 2 * qj + wj - 1
                    dy, dx = y // 4, x // 4
                    y, x = y % 4, x % 4
                    row = (((y // 2) * 2 + x // 2) * 4 + (y % 2) * 2 + x % 2) * ch
                    off = GUARD + (dy + y // 2) * W + dx
                    p1b[(wi * 4 + wj) * ch : (wi * 4 + wj + 1) * ch, :] = s5[row : row + ch, :][
                        :, off : off + n4
                    ].astype(BF16)
            g[qi, qj] = jnp.dot(w1b[...], p1b[...], preferred_element_type=F32)
    for s in range(0, S, 2):
        for c in range(3):
            for i in range(R):
                for qi in range(2):
                    parts = []
                    for e in range(2):
                        q = s + e
                        r = ((q % 8) * 3 + c) * 8
                        lane = i * W + HJ
                        parts.append(g[qi, q // 8, r : r + 8, lane : lane + C])
                    row = c * R * S + i * S + qi * 8
                    flat[row : row + 8, s * C : (s + 2) * C] = jnp.concatenate(parts, axis=1)
    K = S * C
    tile = 256
    for t in range(K // tile):
        p = lax.broadcasted_iota(jnp.int32, (tile, K), 0) + t * tile
        n = lax.broadcasted_iota(jnp.int32, (tile, K), 1)
        group = p // C
        sel[t * tile : (t + 1) * tile, :] = jnp.where(n == (p - group * C) * S + group, 1.0, 0.0).astype(BF16)
    v = flat[...]
    high = v.astype(BF16)
    low = (v - high.astype(F32)).astype(BF16)
    flat[...] = jnp.dot(high, sel[...], preferred_element_type=F32) + jnp.dot(
        low, sel[...], preferred_element_type=F32
    )
    for c in range(3):
        out[c] = flat[c * R * S : (c + 1) * R * S, :] / SPREADS[c]


def swap(a, b, axis):
    count = lax.axis_size(axis)
    first = lax.ppermute(a, axis, [(i, i ^ 1) for i in range(count)])
    second = [(i, (i + 1) % count) for i in range(1, count, 2)]
    second = second + [(j, i) for i, j in second]
    return first, lax.ppermute(b, axis, second)


def neighbours(values, dim, width, axis, where, count):
    even = where % 2 == 0
    size = values.shape[dim]
    head = lax.slice_in_dim(values, 0, width, axis=dim)
    tail = lax.slice_in_dim(values, size - width, size, axis=dim)
    a, b = swap(jnp.where(even, tail, head), jnp.where(even, head, tail), axis)
    zero = jnp.zeros_like(head)
    before = jnp.where(where > 0, jnp.where(even, b, a), zero)
    after = jnp.where(where < count - 1, jnp.where(even, a, b), zero)
    return before, after


def call(kernel, outs, scratch, *args):
    specs = [pl.BlockSpec(memory_space=pltpu.SMEM if a.ndim == 1 else pltpu.VMEM) for a in args]
    return pl.pallas_call(
        kernel,
        out_shape=outs,
        in_specs=specs,
        out_specs=jax.tree.map(lambda _: pl.BlockSpec(memory_space=pltpu.VMEM), outs),
        scratch_shapes=scratch,
        compiler_params=pltpu.CompilerParams(vmem_limit_bytes=56 * 2**20),
    )(*args)


def local(
    image_gen, image_ref, kernel_one, bias_one, kernel_two, bias_two, kernel_three, bias_three,
    lin_first, lin_second, lin_third,
):
    R = image_gen.shape[1] // S
    C = image_gen.shape[2] // S
    W = C + 2 * HJ
    high = lax.axis_size("row") * lax.axis_size("chan")
    across = lax.axis_size("col")
    at_row = lax.axis_index("row") * lax.axis_size("chan") + lax.axis_index("chan")
    at_col = lax.axis_index("col")
    pixels = image_gen.shape[1] * image_gen.shape[2] * high * across
    ch1, ch2, ch3 = bias_one.shape[0], bias_two.shape[0], bias_three.shape[0]

    offsets = jnp.array(OFFSETS, F32)[:, None, None]
    spreads = jnp.array(SPREADS, F32)[:, None, None]
    both = jnp.stack([((image - offsets) / spreads).astype(BF16) for image in (image_gen, image_ref)])
    left, right = neighbours(both, 3, HJ * S, "col", at_col, across)
    rim = jnp.concatenate([left, both, right], axis=3)
    over, under = neighbours(rim, 2, RIM, ROWS, at_row, high)
    rim = jnp.concatenate([over, rim, under], axis=2)
    span = (W + 4) * S
    rim = jnp.pad(rim, ((0, 0), (0, 0), (0, 0), (0, span - W * S)))
    rim = rim.reshape(2, 3 * (R * S + 2 * RIM), span)

    y, x, c, a, b = np.meshgrid(*(np.arange(n) for n in (3, 3, 3, 4, 4)), indexing="ij")
    want = jnp.asarray((x * 192 + b * 48 + c * 16 + y * 4 + a).reshape(1, -1), jnp.int32)
    place = jnp.stack([at_row, at_col]).astype(jnp.int32)
    shard = kernel_three.shape[3]

    def arr(shape, dtype=F32):
        return jax.ShapeDtypeStruct(shape, dtype)

    w1, w1b, w2, w2b, mine, masks = call(
        functools.partial(weights_kernel, R, C, high, across),
        (
            arr((4 * ch1, 768), BF16),
            arr((192, 16 * ch1), BF16),
            arr((4 * ch2, 36 * ch1), BF16),
            arr((4 * ch1, 36 * ch2), BF16),
            arr((shard, 9 * ch2), BF16),
            arr((16, 1024)),
        ),
        [pltpu.VMEM((976, ch1), F32)],
        place, want, kernel_one.reshape(-1, ch1), kernel_two, kernel_three.reshape(-1, shard),
    )
    parts = lax.axis_size("chan")
    whole = mine[None]
    step = 1
    here = lax.axis_index("chan")
    while step < parts:
        other = lax.ppermute(whole, "chan", [(i, i ^ step) for i in range(parts)])
        first = (here & step) == 0
        whole = jnp.concatenate([jnp.where(first, whole, other), jnp.where(first, other, whole)])
        step *= 2
    w3 = whole.reshape(ch3, 9 * ch2)

    def flat(values):
        return values.reshape(1, -1)

    b1, b2, b3 = flat(bias_one), flat(bias_two), flat(bias_three)
    lin1, lin2, lin3 = flat(lin_first), flat(lin_second), flat(lin_third)

    frame = up128((R + 1) * W)
    n2, n3, n4 = up128((R + 4) * W), up128((R + 2) * W), up128(R * W)
    rows = 3 * (R * S + 2 * RIM)

    pre, pool, msg_a, msg_b = call(
        functools.partial(cells_kernel, R, C),
        (
            arr((2, 2, 4 * ch1, 2 * frame)),
            arr((8 * ch1, n4), BF16),
            arr((8 * ch1, up128(3 * W)), BF16),
            arr((8 * ch1, up128(3 * W)), BF16),
        ),
        [pltpu.VMEM((span, span), BF16), pltpu.VMEM((2, rows, span), F32), pltpu.VMEM((768, 2 * frame), BF16)],
        place, rim, w1, b1, masks,
    )
    rec_a, rec_b = swap(msg_a, msg_b, ROWS)
    base, gain, loss1, w3b = call(
        functools.partial(first_grad_kernel, R, C),
        (arr((2, 2, 4 * ch1, frame)), arr((2, 2, 4 * ch1, frame)), arr((8, frame)), arr((ch2, 9 * ch3), BF16)),
        [],
        pre, lin1, masks, w3,
    )
    ext1 = GUARD + up128((R + 6) * W) + GUARD
    d2, msg_a, msg_b, loss2, loss3 = call(
        functools.partial(middle_kernel, R, C),
        (
            arr((4 * ch2, n4), BF16),
            arr((4 * ch2, up128(2 * W)), BF16),
            arr((4 * ch2, up128(2 * W)), BF16),
            arr((8, n4)),
            arr((8, 128)),
        ),
        [
            pltpu.VMEM((8 * ch1, ext1), F32),
            pltpu.VMEM((36 * ch1, 2 * n2), BF16),
            pltpu.VMEM((4 * ch2, 2 * n2), F32),
            pltpu.VMEM((ch2, 2 * n2), F32),
            pltpu.VMEM((2 * ch2, GUARD + n2 + GUARD), F32),
            pltpu.VMEM((9 * ch2, 2 * n3), BF16),
            pltpu.VMEM((ch3, 2 * n3), F32),
            pltpu.VMEM((ch3, GUARD + n3 + GUARD), F32),
            pltpu.VMEM((9 * ch3, n4), BF16),
        ],
        place, pool, rec_a, rec_b, masks, w2, b2, lin2, w3, b3, lin3, w3b,
    )
    rec_a, rec_b = swap(msg_a, msg_b, ROWS)
    partial_loss = (
        jnp.sum(loss1[0]) / (pixels // 16) + jnp.sum(loss2[0]) / (pixels // 64) + jnp.sum(loss3[0]) / (pixels // 256)
    )
    everyone = high * across
    spread_out = jnp.broadcast_to(partial_loss, (everyone, 8, 128))
    loss = jnp.sum(lax.all_to_all(spread_out, ("row", "col", "chan"), 0, 0)[:, 0, 0])
    image_grad = call(
        functools.partial(last_kernel, R, C),
        arr(image_gen.shape),
        [
            pltpu.VMEM((4 * ch2, GUARD + up128((R + 4) * W) + GUARD), F32),
            pltpu.VMEM((36 * ch2, frame), BF16),
            pltpu.VMEM((16 * ch1, GUARD + frame + GUARD), F32),
            pltpu.VMEM((16 * ch1, n4), BF16),
            pltpu.VMEM((2, 2, 192, n4), F32),
            pltpu.VMEM((S * C, S * C), BF16),
            pltpu.VMEM((3 * R * S, S * C), F32),
        ],
        place, d2, rec_a, rec_b, masks, w2b, base, gain, w1b,
    )
    return image_grad, loss


def solution(mesh):
    tile = P(None, ROWS, "col")
    return jax.shard_map(
        local,
        mesh=mesh,
        in_specs=(tile, tile, P(), P(), P(), P(), P(None, None, None, "chan"), P(), P(), P(), P()),
        out_specs=(tile, P()),
        check_vma=False,
    )
```

```python
import functools

import jax
import jax.numpy as jnp
import numpy as np
from jax import lax
from jax.experimental import pallas as pl
from jax.experimental.pallas import tpu as pltpu
from jax.sharding import PartitionSpec as P

OFFSETS = (-0.03, -0.088, -0.188)
SPREADS = (0.458, 0.448, 0.45)
EPSILON = 1e-06

S = 16
HJ = 6
RIM = 12
F32 = jnp.float32
BF16 = jnp.bfloat16
ROWS = ("row", "chan")
GUARD = 128


def up128(n):
    return -(-n // 128) * 128


def wide(column, lanes):
    return jnp.concatenate([column] * (lanes // 128), axis=1)


def column(row, times=1):
    n = row.shape[1]
    here = lax.broadcasted_iota(jnp.int32, (n, n), 0) == lax.broadcasted_iota(jnp.int32, (n, n), 1)
    one = jnp.sum(jnp.where(here, jnp.broadcast_to(row[...], (n, n)), 0.0), axis=1, keepdims=True)
    one = jnp.broadcast_to(one, (n, 128))
    return jnp.concatenate([one] * times, axis=0) if times > 1 else one


def sigmoid(v):
    return 0.5 + 0.5 * jnp.tanh(0.5 * v)


def lanes_of(values, start, count, total):
    part = values[:, start : start + count]
    if total == count:
        return part
    return jnp.concatenate([part, jnp.zeros((values.shape[0], total - count), values.dtype)], axis=1)


def layer_terms(v0, v1, lin, factor):
    g0 = sigmoid(v0)
    f0 = v0 * g0
    f1 = v1 * sigmoid(v1)
    s0 = lax.rsqrt(jnp.sum(f0 * f0, axis=0, keepdims=True) + EPSILON)
    s1 = lax.rsqrt(jnp.sum(f1 * f1, axis=0, keepdims=True) + EPSILON)
    diff = f0 * s0 - f1 * s1
    weighted = lin * diff
    slope = (2.0 * factor) * weighted
    inner = jnp.sum(f0 * slope, axis=0, keepdims=True)
    dfeat = s0 * slope - f0 * (s0 * s0 * s0 * inner)
    return dfeat, g0 * (1.0 + v0 * (1.0 - g0)), jnp.sum(weighted * diff, axis=0, keepdims=True)


def shift_all(dst, dst_lane, src, src_row, count, starts, width, chunk=64):
    def body(i, carry):
        part = src[pl.ds(pl.multiple_of(src_row + i * chunk, chunk), chunk), :]
        for n, start in enumerate(starts):
            row = pl.multiple_of(n * count + i * chunk, chunk)
            dst[pl.ds(row, chunk), dst_lane : dst_lane + width] = part[:, start : start + width]
        return carry

    lax.fori_loop(0, count // chunk, body, 0)


def window(W, rows):
    return [GUARD + i * W + j - 1 for i in range(rows) for j in range(3)]


def weights_kernel(R, C, high, across, place, want, k1, k2, w1, w1b, w2_out, w2b_out, masks, t1, w2, w2b, sems):
    taps = k1.shape[0]
    ch1 = k1.shape[1]
    pick = lax.broadcasted_iota(jnp.int32, (768, taps), 0) == want[...]
    t1[200:968, :] = jnp.dot(jnp.where(pick, 1.0, 0.0).astype(BF16), k1[...], preferred_element_type=F32)
    t1[0:200, :] = jnp.zeros((200, ch1), F32)
    t1[968:, :] = jnp.zeros((t1.shape[0] - 968, ch1), F32)
    for ci in range(2):
        for cj in range(2):
            moved = t1[200 - cj * 192 - ci * 4 : 968 - cj * 192 - ci * 4, :]
            row = (ci * 2 + cj) * ch1
            w1[row : row + ch1, :] = moved.T.astype(BF16)
    for wi in range(4):
        low = 200 - 4 * (wi % 2)
        half = 1 if wi < 2 else 0
        for wj in range(0, 4, 2):
            parts = []
            for e in range(2):
                start = low + (2 - wj - e) * 192
                block = t1[start : start + 384, :].reshape(24, 2, 8, ch1)[:, half]
                parts.append(block.reshape(192, ch1))
            lane = (wi * 4 + wj) * ch1
            w1b[:, lane : lane + 2 * ch1] = jnp.concatenate(parts, axis=1).astype(BF16)
    size = 5
    ch2 = k2.shape[3]
    none = jnp.zeros((ch1, ch2), F32)

    def tap(y, x):
        return k2[y, x].astype(F32) if 0 <= x < size else none

    for pi in range(2):
        w = 5 * (1 - pi)
        lane = (w // 2) * 12 + (w % 2) * 2
        for x in range(3):
            a = (lane + 4 * x) * ch1
            w2[pi * 2 * ch2 : (pi + 1) * 2 * ch2, a : a + 2 * ch1] = jnp.zeros((2 * ch2, 2 * ch1), BF16)
            a = (lane + 4 * x) * ch2
            w2b[pi * 2 * ch1 : (pi + 1) * 2 * ch1, a : a + 2 * ch2] = jnp.zeros((2 * ch1, 2 * ch2), BF16)
    copies = []
    for pj in range(2):
        for y in range(size):
            for x in range(3):
                pair = jnp.concatenate([tap(y, 2 * x - pj), tap(y, 2 * x + 1 - pj)], axis=0).T.astype(BF16)
                for pi in range(2):
                    w = y + pi
                    lane = ((w // 2) * 3 + x) * 4 + (w % 2) * 2
                    row = (pi * 2 + pj) * ch2
                    w2[row : row + ch2, lane * ch1 : (lane + 2) * ch1] = pair
        for pi in range(2):
            rows = pl.ds((pi * 2 + pj) * ch2, ch2)
            copies.append(pltpu.make_async_copy(w2.at[rows], w2_out.at[rows], sems.at[len(copies)]))
            copies[-1].start()
    for pj in range(2):
        for y in range(size):
            for x in range(3):
                back = jnp.concatenate(
                    [tap(size - 1 - y, size - 1 - 2 * x + pj), tap(size - 1 - y, size - 2 - 2 * x + pj)], axis=1
                ).astype(BF16)
                for pi in range(2):
                    w = y + pi
                    lane = ((w // 2) * 3 + x) * 4 + (w % 2) * 2
                    row = (pi * 2 + pj) * ch1
                    w2b[row : row + ch1, lane * ch2 : (lane + 2) * ch2] = back
        for pi in range(2):
            rows = pl.ds((pi * 2 + pj) * ch1, ch1)
            copies.append(pltpu.make_async_copy(w2b.at[rows], w2b_out.at[rows], sems.at[len(copies)]))
            copies[-1].start()
    W = C + 2 * HJ
    lane = lax.broadcasted_iota(jnp.int32, (1, masks.shape[1]), 1)
    i = ((lane.astype(F32) + 0.5) * (1.0 / W)).astype(jnp.int32)
    j = lane - i * W - HJ
    frames = (
        (0, R, False), (0, R + 1, True), (-1, R + 1, True), (-3, R + 6, False), (-2, R + 4, False),
        (-1, R + 2, False), (-1, R + 2, True), (0, R, True), (0, R + 1, False), (-1, R + 1, False),
    )
    masks[...] = jnp.zeros(masks.shape, F32)
    for n, (start, count, mine) in enumerate(frames):
        r, c = i + start, j
        rows, columns = R, C
        if not mine:
            r, c = r + place[0] * R, c + place[1] * C
            rows, columns = R * high, C * across
        ok = (i < count) & (r >= 0) & (r < rows) & (c >= 0) & (c < columns)
        masks[n : n + 1, :] = jnp.where(ok, 1.0, 0.0)
    for copy in copies:
        copy.wait()


def cells_kernel(R, C, par, img, w1, b1, masks, pre, pool, msg_a, msg_b, sel, z, p1):
    W = C + 2 * HJ
    G = W + 4
    frame = up128((R + 1) * W)
    px = W * S
    K = sel.shape[0]
    rows = R * S + 2 * RIM
    tile = 256
    for t in range(K // tile):
        p = lax.broadcasted_iota(jnp.int32, (K, tile), 0)
        n = lax.broadcasted_iota(jnp.int32, (K, tile), 1) + t * tile
        want = (p & (S - 1)) * G + (p >> 4)
        sel[:, t * tile : (t + 1) * tile] = jnp.where((n == want) & (p < px), 1.0, 0.0).astype(BF16)
    for f in range(2):
        for t in range(K // tile):
            z[f, :, t * tile : (t + 1) * tile] = jnp.dot(
                img[f], sel[:, t * tile : (t + 1) * tile], preferred_element_type=F32
            )
    own = masks[0:1, 0 : R * W]
    bias = wide(column(b1, 4), tile)
    for pi in range(2):
        top = 8 - 8 * pi
        for pj in range(2):
            for f in range(2):
                for s in range(S):
                    q = s + 8 * pj - 4
                    lane = (q % S) * G + q // S
                    parts = []
                    for k in range(R + 1):
                        r = top + S * k
                        parts.append(
                            jnp.concatenate(
                                [z[f, c * rows + r : c * rows + r + S, lane : lane + W] for c in range(3)], axis=0
                            )
                        )
                    parts.append(jnp.zeros((3 * S, frame - (R + 1) * W), F32))
                    p1[s * 48 : s * 48 + 48, f * frame : (f + 1) * frame] = jnp.concatenate(parts, axis=1).astype(BF16)
            for t in range(2 * frame // tile):
                lanes = slice(t * tile, (t + 1) * tile)
                pre[pi, pj, :, lanes] = jnp.dot(w1[...], p1[:, lanes], preferred_element_type=F32) + bias
            for f in range(2):
                v = pre[pi, pj, :, f * frame : (f + 1) * frame]
                feat = v * sigmoid(v)
                quarter = feat.shape[0] // 4
                mean = 0.25 * (
                    (feat[0:quarter] + feat[quarter : 2 * quarter])
                    + (feat[2 * quarter : 3 * quarter] + feat[3 * quarter :])
                )
                mine = mean[:, pi * W : pi * W + R * W]
                mine = jnp.where(own > 0.0, mine, 0.0)
                row = (f * 4 + pi * 2 + pj) * quarter
                even = lax.rem(par[0], 2) == 0
                head = lanes_of(mine, 0, 3 * W, msg_a.shape[1])
                tail = lanes_of(mine, (R - 3) * W, 3 * W, msg_a.shape[1])
                msg_a[row : row + quarter, :] = jnp.where(even, tail, head).astype(BF16)
                msg_b[row : row + quarter, :] = jnp.where(even, head, tail).astype(BF16)
                pool[row : row + quarter, :] = lanes_of(mine, 0, R * W, pool.shape[1]).astype(BF16)


def first_grad_kernel(R, C, order, place, pre, lin, masks, b3, lin3, *refs):
    k3, (base, gain, loss, w3, w3b, consts, bias) = refs[: len(order)], refs[len(order) :]
    frame = base.shape[3]
    ch = lin.shape[1]
    c2 = w3b.shape[0]
    c3 = w3.shape[0]
    shard = k3[0].shape[1]
    total = jnp.zeros((1, frame), F32)
    weights = wide(column(lin), frame)
    for pi in range(2):
        for pj in range(2):
            for t in range(4):
                v0 = pre[pi, pj, t * ch : (t + 1) * ch, 0:frame]
                v1 = pre[pi, pj, t * ch : (t + 1) * ch, frame : 2 * frame]
                dfeat, slope, part = layer_terms(v0, v1, weights, 16.0)
                base[pi, pj, t * ch : (t + 1) * ch, :] = dfeat * slope
                gain[pi, pj, t * ch : (t + 1) * ch, :] = 0.25 * slope
                total = total + jnp.where(masks[1 + pi : 2 + pi, 0:frame] > 0.0, part, 0.0)
    loss[...] = jnp.broadcast_to(total, loss.shape)
    bias[0] = column(b3)
    bias[1] = column(lin3)
    for n, flip in enumerate(order):
        start = pl.multiple_of(jnp.bitwise_xor(place[2], flip) * shard, 8)
        for e in range(2):
            consts[e, n * shard : (n + 1) * shard, :] = bias[e, pl.ds(start, shard), :]
        for k in range(0, 9, 2):
            size = min(2, 9 - k) * c2
            taps = k3[n][k * c2 : k * c2 + size, :].astype(F32)
            w3[n * shard : (n + 1) * shard, k * c2 : k * c2 + size] = taps.T.astype(BF16)
    for k in range(9):
        taps = [k3[n][(8 - k) * c2 : (9 - k) * c2, :] for n in range(len(order))]
        w3b[:, k * c3 : (k + 1) * c3] = jnp.concatenate(taps, axis=1)


def middle_kernel(
    R, C, pixels, par, pool, rec_a, rec_b, masks, w2, b2, lin2, w3, consts, w3b, loss1, d2, msg_a, msg_b, loss,
    s1, p2, pre2, q2, s2, p3, pre3, s3, p3b,
):
    W = C + 2 * HJ
    even = lax.rem(par[0], 2) == 0
    n2 = up128((R + 4) * W)
    n3 = up128((R + 2) * W)
    n4 = up128(R * W)
    c1 = pool.shape[0] // 2
    c2 = b2.shape[1]
    c3 = w3.shape[0]
    ext = s1.shape[1]
    inside = masks[3:4, 0 : (R + 6) * W]
    for r in range(0, 2 * c1, 64):
        a = rec_a[r : r + 64, :].astype(F32)
        b = rec_b[r : r + 64, :].astype(F32)
        above = jnp.where(even, b, a)[:, 0 : 3 * W]
        below = jnp.where(even, a, b)[:, 0 : 3 * W]
        mine = pool[r : r + 64, :].astype(F32)[:, 0 : R * W]
        whole = jnp.concatenate([above, mine, below], axis=1)
        whole = jnp.where(inside > 0.0, whole, 0.0)
        s1[r : r + 64, :] = jnp.concatenate(
            [jnp.zeros((64, GUARD), F32), whole, jnp.zeros((64, ext - GUARD - (R + 6) * W), F32)], axis=1
        ).astype(BF16)
    for f in range(2):
        shift_all(p2, f * n2, s1, f * c1, c1, window(W, 3), n2)
    tile = 256
    bias2 = column(b2, 4)
    bias3 = consts[0]
    lins3 = consts[1]

    def second(t, carry):
        lanes = pl.ds(pl.multiple_of(t * tile, tile), tile)
        v = jnp.dot(w2[...], p2[:, lanes], preferred_element_type=F32) + wide(bias2, tile)
        pre2[:, lanes] = v
        feat = v * sigmoid(v)
        q2[:, lanes] = 0.25 * (
            (feat[0:c2] + feat[c2 : 2 * c2]) + (feat[2 * c2 : 3 * c2] + feat[3 * c2 :])
        )
        return carry

    lax.fori_loop(0, 2 * n2 // tile, second, 0)
    for f in range(2):
        good = jnp.where(masks[4:5, 0:n2] > 0.0, q2[:, f * n2 : (f + 1) * n2], 0.0)
        s2[f * c2 : (f + 1) * c2, 0:GUARD] = jnp.zeros((c2, GUARD), BF16)
        s2[f * c2 : (f + 1) * c2, GUARD : GUARD + n2] = good.astype(BF16)
        s2[f * c2 : (f + 1) * c2, GUARD + n2 :] = jnp.zeros((c2, s2.shape[1] - GUARD - n2), BF16)
        shift_all(p3, f * n3, s2, f * c2, c2, window(W, 3), n3)

    def third(t, carry):
        lanes = pl.ds(pl.multiple_of(t * tile, tile), tile)
        pre3[:, lanes] = jnp.dot(w3[...], p3[:, lanes], preferred_element_type=F32) + wide(bias3, tile)
        return carry

    lax.fori_loop(0, 2 * n3 // tile, third, 0)
    s3[:, 0:GUARD] = jnp.zeros((c3, GUARD), BF16)
    s3[:, GUARD + n3 :] = jnp.zeros((c3, s3.shape[1] - GUARD - n3), BF16)
    total = jnp.zeros((1, 128), F32)
    for t in range(n3 // 128):
        v0 = pre3[:, t * 128 : (t + 1) * 128]
        v1 = pre3[:, n3 + t * 128 : n3 + (t + 1) * 128]
        dfeat, slope, part = layer_terms(v0, v1, lins3, 256.0)
        lanes = slice(t * 128, (t + 1) * 128)
        d = jnp.where(masks[5:6, lanes] > 0.0, dfeat * slope, 0.0)
        s3[:, GUARD + t * 128 : GUARD + (t + 1) * 128] = d.astype(BF16)
        total = total + jnp.where(masks[6:7, lanes] > 0.0, part, 0.0)
    shift_all(p3b, 0, s3, 0, c3, window(W, 3), n4)
    up = 0.25 * jnp.dot(w3b[...], p3b[...], preferred_element_type=F32)
    total2 = jnp.zeros((1, n4), F32)
    weights = wide(column(lin2), n4)
    strips = []
    for t in range(4):
        rows = slice(t * c2, (t + 1) * c2)
        v0 = pre2[rows, 0:n2][:, 2 * W : 2 * W + n4]
        v1 = pre2[rows, n2 : 2 * n2][:, 2 * W : 2 * W + n4]
        dfeat, slope, part = layer_terms(v0, v1, weights, 64.0)
        d = jnp.where(masks[0:1, 0:n4] > 0.0, (dfeat + up) * slope, 0.0)
        d2[rows, :] = d.astype(BF16)
        total2 = total2 + jnp.where(masks[7:8, 0:n4] > 0.0, part, 0.0)
        strips.append(d)
    rest = jnp.zeros((c2, msg_a.shape[1] - 3 * W), F32)
    for pj in range(2):
        upper, lower = strips[pj], strips[2 + pj]
        head = jnp.concatenate([upper[:, 0:W], lower[:, 0:W], upper[:, W : 2 * W], rest], axis=1)
        tail = jnp.concatenate(
            [lower[:, (R - 2) * W : (R - 1) * W], upper[:, (R - 1) * W : R * W], lower[:, (R - 1) * W : R * W], rest],
            axis=1,
        )
        rows = slice(pj * c2, (pj + 1) * c2)
        msg_a[rows, :] = jnp.where(even, tail, head).astype(BF16)
        msg_b[rows, :] = jnp.where(even, head, tail).astype(BF16)
    each = (
        jnp.sum(loss1[0:1, :]) / (pixels // 16) + jnp.sum(total2) / (pixels // 64) + jnp.sum(total) / (pixels // 256)
    )
    loss[...] = jnp.full(loss.shape, each, F32)


def last_kernel(
    R, C, par, d2, rec_a, rec_b, masks, w2b_in, base_in, gain_in, w1b_in, out,
    s4, p2b, s5, p1b, g, sel, flat, w2b, base, gain, w1b, sems,
):
    pairs = ((w2b_in, w2b), (base_in, base), (gain_in, gain), (w1b_in, w1b))
    fetch = [pltpu.make_async_copy(a, b, sems.at[n]) for n, (a, b) in enumerate(pairs)]
    for copy in fetch:
        copy.start()
    W = C + 2 * HJ
    even = lax.rem(par[0], 2) == 0
    c2 = d2.shape[0]
    frame = base.shape[3]
    n4 = up128(R * W)
    ext = s4.shape[1]
    ch = w2b.shape[0] // 4
    inside = masks[4:5, 0 : (R + 4) * W]

    none = jnp.zeros((64, W), F32)
    for t in range(0, c2, 64):
        pi, row = t // (c2 // 2), t % (c2 // 2)
        a = rec_a[row : row + 64, :].astype(F32)
        b = rec_b[row : row + 64, :].astype(F32)
        above = jnp.where(even, b, a)
        below = jnp.where(even, a, b)
        strips = [[v[:, n * W : (n + 1) * W] for n in range(3)] for v in (above, below)]
        mine = d2[t : t + 64, :].astype(F32)[:, 0 : R * W]
        if pi == 0:
            parts = [none, strips[0][1], mine, strips[1][0], strips[1][2]]
        else:
            parts = [strips[0][0], strips[0][2], mine, strips[1][1], none]
        whole = jnp.where(inside > 0.0, jnp.concatenate(parts, axis=1), 0.0)
        s4[t : t + 64, :] = jnp.concatenate(
            [jnp.zeros((64, GUARD), F32), whole, jnp.zeros((64, ext - GUARD - (R + 4) * W), F32)], axis=1
        ).astype(BF16)
    shift_all(p2b, 0, s4, 0, c2, window(W, 4), frame)
    for copy in fetch:
        copy.wait()
    for qi in range(2):
        around = p2b[(1 - qi) * 3 * c2 : (4 - qi) * 3 * c2, :]
        up = jnp.dot(w2b[qi * 2 * ch : (qi + 1) * 2 * ch, :], around, preferred_element_type=F32)
        good = masks[8 + qi : 9 + qi, 0:frame] > 0.0
        for qj in range(2):
            part = up[qj * ch : (qj + 1) * ch]
            for t in range(4):
                rows = slice(t * ch, (t + 1) * ch)
                d = base[qi, qj, rows, :] + gain[qi, qj, rows, :] * part
                row = ((qi * 2 + qj) * 4 + t) * ch
                s5[row : row + ch, 0:GUARD] = jnp.zeros((ch, GUARD), BF16)
                s5[row : row + ch, GUARD : GUARD + frame] = jnp.where(good, d, 0.0).astype(BF16)
                s5[row : row + ch, GUARD + frame :] = jnp.zeros((ch, s5.shape[1] - GUARD - frame), BF16)
    for qi in range(2):
        for qj in range(2):
            for wi in range(4):
                for wj in range(4):
                    y, x = 2 * qi + wi - 1, 2 * qj + wj - 1
                    dy, dx = y // 4, x // 4
                    y, x = y % 4, x % 4
                    row = (((y // 2) * 2 + x // 2) * 4 + (y % 2) * 2 + x % 2) * ch
                    off = GUARD + (dy + y // 2) * W + dx
                    p1b[(wi * 4 + wj) * ch : (wi * 4 + wj + 1) * ch, :] = s5[row : row + ch, :][
                        :, off : off + n4
                    ]
            g[qi, qj] = jnp.dot(w1b[...], p1b[...], preferred_element_type=F32)
    for s in range(0, S, 2):
        for c in range(3):
            for i in range(R):
                for qi in range(2):
                    parts = []
                    for e in range(2):
                        q = s + e
                        r = ((q % 8) * 3 + c) * 8
                        lane = i * W + HJ
                        parts.append(g[qi, q // 8, r : r + 8, lane : lane + C])
                    row = c * R * S + i * S + qi * 8
                    flat[row : row + 8, s * C : (s + 2) * C] = jnp.concatenate(parts, axis=1)
    K = S * C
    tile = 256
    for t in range(K // tile):
        p = lax.broadcasted_iota(jnp.int32, (tile, K), 0) + t * tile
        n = lax.broadcasted_iota(jnp.int32, (tile, K), 1)
        group = p // C
        sel[t * tile : (t + 1) * tile, :] = jnp.where(n == (p - group * C) * S + group, 1.0, 0.0).astype(BF16)
    v = flat[...]
    high = v.astype(BF16)
    low = (v - high.astype(F32)).astype(BF16)
    flat[...] = jnp.dot(high, sel[...], preferred_element_type=F32) + jnp.dot(
        low, sel[...], preferred_element_type=F32
    )
    for c in range(3):
        out[c] = flat[c * R * S : (c + 1) * R * S, :] / SPREADS[c]


def swap(a, b, axis):
    count = lax.axis_size(axis)
    first = lax.ppermute(a, axis, [(i, i ^ 1) for i in range(count)])
    second = [(i, (i + 1) % count) for i in range(1, count, 2)]
    second = second + [(j, i) for i, j in second]
    return first, lax.ppermute(b, axis, second)


def neighbours(values, dim, width, axis, where, count):
    even = where % 2 == 0
    size = values.shape[dim]
    head = lax.slice_in_dim(values, 0, width, axis=dim)
    tail = lax.slice_in_dim(values, size - width, size, axis=dim)
    a, b = swap(jnp.where(even, tail, head), jnp.where(even, head, tail), axis)
    zero = jnp.zeros_like(head)
    before = jnp.where(where > 0, jnp.where(even, b, a), zero)
    after = jnp.where(where < count - 1, jnp.where(even, a, b), zero)
    return before, after


class Far:
    def __init__(self, array):
        self.array = array


def call(kernel, outs, scratch, limit, work, *args, far=()):
    def place(a):
        if isinstance(a, Far):
            return pltpu.HBM
        return pltpu.SMEM if a.ndim == 1 else pltpu.VMEM

    specs = [pl.BlockSpec(memory_space=place(a)) for a in args]
    args = [a.array if isinstance(a, Far) else a for a in args]
    spaces = [pltpu.HBM if n in far else pltpu.VMEM for n in range(len(jax.tree.leaves(outs)))]
    out_specs = jax.tree.unflatten(jax.tree.structure(outs), [pl.BlockSpec(memory_space=m) for m in spaces])
    return pl.pallas_call(
        kernel,
        out_shape=outs,
        in_specs=specs,
        out_specs=out_specs,
        scratch_shapes=scratch,
        compiler_params=pltpu.CompilerParams(vmem_limit_bytes=limit * 2**20),
        cost_estimate=pl.CostEstimate(flops=work * 10**9, bytes_accessed=2**20, transcendentals=0),
    )(*args)


def local(
    image_gen, image_ref, kernel_one, bias_one, kernel_two, bias_two, kernel_three, bias_three,
    lin_first, lin_second, lin_third,
):
    R = image_gen.shape[1] // S
    C = image_gen.shape[2] // S
    W = C + 2 * HJ
    high = lax.axis_size("row") * lax.axis_size("chan")
    across = lax.axis_size("col")
    at_row = lax.axis_index("row") * lax.axis_size("chan") + lax.axis_index("chan")
    at_col = lax.axis_index("col")
    pixels = image_gen.shape[1] * image_gen.shape[2] * high * across
    ch1, ch2, ch3 = bias_one.shape[0], bias_two.shape[0], bias_three.shape[0]

    y, x, c, a, b = np.meshgrid(*(np.arange(n) for n in (3, 3, 3, 4, 4)), indexing="ij")
    want = jnp.asarray((x * 192 + b * 48 + c * 16 + y * 4 + a).reshape(1, -1), jnp.int32)
    place = jnp.stack([at_row, at_col, lax.axis_index("chan")]).astype(jnp.int32)
    shard = kernel_three.shape[3]

    def arr(shape, dtype=F32):
        return jax.ShapeDtypeStruct(shape, dtype)

    w1, w1b, w2, w2b, masks = call(
        functools.partial(weights_kernel, R, C, high, across),
        (
            arr((4 * ch1, 768), BF16),
            arr((192, 16 * ch1), BF16),
            arr((4 * ch2, 36 * ch1), BF16),
            arr((4 * ch1, 36 * ch2), BF16),
            arr((16, 1024)),
        ),
        [
            pltpu.VMEM((976, ch1), F32),
            pltpu.VMEM((4 * ch2, 36 * ch1), BF16),
            pltpu.VMEM((4 * ch1, 36 * ch2), BF16),
            pltpu.SemaphoreType.DMA((8,)),
        ],
        62, 5, place, want, kernel_one.reshape(-1, ch1), kernel_two, far=(2, 3),
    )
    parts = lax.axis_size("chan")
    pieces = [kernel_three.reshape(-1, shard)]
    order = [0]
    step = parts // 2
    while step > 0:
        pairs = [(i, i ^ step) for i in range(parts)]
        pieces = pieces + [lax.ppermute(piece, "chan", pairs) for piece in pieces]
        order = order + [n ^ step for n in order]
        step //= 2

    offsets = jnp.array(OFFSETS, F32)[:, None, None]
    spreads = jnp.array(SPREADS, F32)[:, None, None]
    both = jnp.stack([((image - offsets) / spreads).astype(BF16) for image in (image_gen, image_ref)])
    left, right = neighbours(both, 3, HJ * S, "col", at_col, across)
    rim = jnp.concatenate([left, both, right], axis=3)
    over, under = neighbours(rim, 2, RIM, ROWS, at_row, high)
    rim = jnp.concatenate([over, rim, under], axis=2)
    span = (W + 4) * S
    rim = jnp.pad(rim, ((0, 0), (0, 0), (0, 0), (0, span - W * S)))
    rim = rim.reshape(2, 3 * (R * S + 2 * RIM), span)

    def flat(values):
        return values.reshape(1, -1)

    b1, b2, b3 = flat(bias_one), flat(bias_two), flat(bias_three)
    lin1, lin2, lin3 = flat(lin_first), flat(lin_second), flat(lin_third)

    frame = up128((R + 1) * W)
    n2, n3, n4 = up128((R + 4) * W), up128((R + 2) * W), up128(R * W)
    rows = 3 * (R * S + 2 * RIM)

    pre, pool, msg_a, msg_b = call(
        functools.partial(cells_kernel, R, C),
        (
            arr((2, 2, 4 * ch1, 2 * frame)),
            arr((8 * ch1, n4), BF16),
            arr((8 * ch1, up128(3 * W)), BF16),
            arr((8 * ch1, up128(3 * W)), BF16),
        ),
        [pltpu.VMEM((span, span), BF16), pltpu.VMEM((2, rows, span), F32), pltpu.VMEM((768, 2 * frame), BF16)],
        18, 5, place, rim, w1, b1, masks,
    )
    rec_a, rec_b = swap(msg_a, msg_b, ROWS)
    base, gain, loss1, w3, w3b, consts = call(
        functools.partial(first_grad_kernel, R, C, tuple(order)),
        (arr((2, 2, 4 * ch1, frame)), arr((2, 2, 4 * ch1, frame)), arr((8, frame)),
            arr((ch3, 9 * ch2), BF16), arr((ch2, 9 * ch3), BF16), arr((2, ch3, 128))),
        [pltpu.VMEM((2, ch3, 128), F32)],
        12, 3, place, pre, lin1, masks, b3, lin3, *pieces,
    )
    ext1 = GUARD + up128((R + 6) * W) + GUARD
    everyone = high * across
    d2, msg_a, msg_b, each = call(
        functools.partial(middle_kernel, R, C, pixels),
        (
            arr((4 * ch2, n4), BF16),
            arr((2 * ch2, up128(3 * W)), BF16),
            arr((2 * ch2, up128(3 * W)), BF16),
            arr((everyone, 8, 128)),
        ),
        [
            pltpu.VMEM((8 * ch1, ext1), BF16),
            pltpu.VMEM((36 * ch1, 2 * n2), BF16),
            pltpu.VMEM((4 * ch2, 2 * n2), F32),
            pltpu.VMEM((ch2, 2 * n2), F32),
            pltpu.VMEM((2 * ch2, GUARD + n2 + GUARD), BF16),
            pltpu.VMEM((9 * ch2, 2 * n3), BF16),
            pltpu.VMEM((ch3, 2 * n3), F32),
            pltpu.VMEM((ch3, GUARD + n3 + GUARD), BF16),
            pltpu.VMEM((9 * ch3, n4), BF16),
        ],
        30, 10, place, pool, rec_a, rec_b, masks, w2, b2, lin2, w3, consts, w3b, loss1,
    )
    rec_a, rec_b = swap(msg_a, msg_b, ROWS)
    with jax.named_scope("share"):
        everywhere = lax.all_to_all(each, ("row", "col", "chan"), 0, 0)
    image_grad = call(
        functools.partial(last_kernel, R, C),
        arr(image_gen.shape),
        [
            pltpu.VMEM((4 * ch2, GUARD + up128((R + 4) * W) + GUARD), BF16),
            pltpu.VMEM((48 * ch2, frame), BF16),
            pltpu.VMEM((16 * ch1, GUARD + frame + GUARD), BF16),
            pltpu.VMEM((16 * ch1, n4), BF16),
            pltpu.VMEM((2, 2, 192, n4), F32),
            pltpu.VMEM((S * C, S * C), BF16),
            pltpu.VMEM((3 * R * S, S * C), F32),
            pltpu.VMEM(w2b.shape, BF16),
            pltpu.VMEM(base.shape, F32),
            pltpu.VMEM(gain.shape, F32),
            pltpu.VMEM(w1b.shape, BF16),
            pltpu.SemaphoreType.DMA((4,)),
        ],
        62, 10, place, d2, rec_a, rec_b, masks, Far(w2b), Far(base), Far(gain), Far(w1b),
    )
    everywhere, image_grad = lax.optimization_barrier((everywhere, image_grad))
    return image_grad, jnp.sum(everywhere[:, 0, 0])


def solution(mesh):
    tile = P(None, ROWS, "col")
    return jax.shard_map(
        local,
        mesh=mesh,
        in_specs=(tile, tile, P(), P(), P(), P(), P(None, None, None, "chan"), P(), P(), P(), P()),
        out_specs=(tile, P()),
        check_vma=False,
    )
```

```python
import functools

import jax
import jax.numpy as jnp
import numpy as np
from jax import lax
from jax.experimental import pallas as pl
from jax.experimental.pallas import tpu as pltpu
from jax.sharding import PartitionSpec as P


OFFSETS = (-0.03, -0.088, -0.188)
SPREADS = (0.458, 0.448, 0.45)
EPSILON = 1e-06

S = 16
HJ = 6
RIM = 12
F32 = jnp.float32
BF16 = jnp.bfloat16
ROWS = ("row", "chan")
GUARD = 128


def up128(n):
    return -(-n // 128) * 128


def wide(column, lanes):
    return jnp.concatenate([column] * (lanes // 128), axis=1)


def column(row, times=1):
    n = row.shape[1]
    here = lax.broadcasted_iota(jnp.int32, (n, n), 0) == lax.broadcasted_iota(jnp.int32, (n, n), 1)
    one = jnp.sum(jnp.where(here, jnp.broadcast_to(row[...], (n, n)), 0.0), axis=1, keepdims=True)
    one = jnp.broadcast_to(one, (n, 128))
    return jnp.concatenate([one] * times, axis=0) if times > 1 else one


def sigmoid(v):
    return 0.5 + 0.5 * jnp.tanh(0.5 * v)


def lanes_of(values, start, count, total):
    part = values[:, start : start + count]
    if total == count:
        return part
    return jnp.concatenate([part, jnp.zeros((values.shape[0], total - count), values.dtype)], axis=1)


def layer_terms(v0, v1, lin, factor):
    g0 = sigmoid(v0)
    f0 = v0 * g0
    f1 = v1 * sigmoid(v1)
    s0 = lax.rsqrt(jnp.sum(f0 * f0, axis=0, keepdims=True) + EPSILON)
    s1 = lax.rsqrt(jnp.sum(f1 * f1, axis=0, keepdims=True) + EPSILON)
    diff = f0 * s0 - f1 * s1
    weighted = lin * diff
    slope = (2.0 * factor) * weighted
    inner = jnp.sum(f0 * slope, axis=0, keepdims=True)
    dfeat = s0 * slope - f0 * (s0 * s0 * s0 * inner)
    return dfeat, g0 * (1.0 + v0 * (1.0 - g0)), jnp.sum(weighted * diff, axis=0, keepdims=True)


def shift_all(dst, dst_lane, src, src_row, count, starts, width, chunk=64):
    def body(i, carry):
        part = src[pl.ds(pl.multiple_of(src_row + i * chunk, chunk), chunk), :]
        for n, start in enumerate(starts):
            row = pl.multiple_of(n * count + i * chunk, chunk)
            dst[pl.ds(row, chunk), dst_lane : dst_lane + width] = part[:, start : start + width]
        return carry

    lax.fori_loop(0, count // chunk, body, 0)


def window(W, rows):
    return [GUARD + i * W + j - 1 for i in range(rows) for j in range(3)]


def weights_kernel(R, C, high, across, place, want, k1, k2, w1, w1b, w2_out, w2b_out, masks, t1, w2, w2b, sems):
    taps = k1.shape[0]
    ch1 = k1.shape[1]
    pick = lax.broadcasted_iota(jnp.int32, (768, taps), 0) == want[...]
    t1[200:968, :] = jnp.dot(jnp.where(pick, 1.0, 0.0).astype(BF16), k1[...], preferred_element_type=F32)
    t1[0:200, :] = jnp.zeros((200, ch1), F32)
    t1[968:, :] = jnp.zeros((t1.shape[0] - 968, ch1), F32)
    for ci in range(2):
        for cj in range(2):
            moved = t1[200 - cj * 192 - ci * 4 : 968 - cj * 192 - ci * 4, :]
            row = (ci * 2 + cj) * ch1
            w1[row : row + ch1, :] = moved.T.astype(BF16)
    for wi in range(4):
        low = 200 - 4 * (wi % 2)
        half = 1 if wi < 2 else 0
        for wj in range(0, 4, 2):
            parts = []
            for e in range(2):
                start = low + (2 - wj - e) * 192
                block = t1[start : start + 384, :].reshape(24, 2, 8, ch1)[:, half]
                parts.append(block.reshape(192, ch1))
            lane = (wi * 4 + wj) * ch1
            w1b[:, lane : lane + 2 * ch1] = jnp.concatenate(parts, axis=1).astype(BF16)
    size = 5
    ch2 = k2.shape[3]
    none = jnp.zeros((ch1, ch2), F32)

    def tap(y, x):
        return k2[y, x].astype(F32) if 0 <= x < size else none

    for pi in range(2):
        w = 5 * (1 - pi)
        lane = (w // 2) * 12 + (w % 2) * 2
        for x in range(3):
            a = (lane + 4 * x) * ch1
            w2[pi * 2 * ch2 : (pi + 1) * 2 * ch2, a : a + 2 * ch1] = jnp.zeros((2 * ch2, 2 * ch1), BF16)
            a = (lane + 4 * x) * ch2
            w2b[pi * 2 * ch1 : (pi + 1) * 2 * ch1, a : a + 2 * ch2] = jnp.zeros((2 * ch1, 2 * ch2), BF16)
    copies = []
    for pj in range(2):
        for y in range(size):
            for x in range(3):
                pair = jnp.concatenate([tap(y, 2 * x - pj), tap(y, 2 * x + 1 - pj)], axis=0).T.astype(BF16)
                for pi in range(2):
                    w = y + pi
                    lane = ((w // 2) * 3 + x) * 4 + (w % 2) * 2
                    row = (pi * 2 + pj) * ch2
                    w2[row : row + ch2, lane * ch1 : (lane + 2) * ch1] = pair
        for pi in range(2):
            rows = pl.ds((pi * 2 + pj) * ch2, ch2)
            copies.append(pltpu.make_async_copy(w2.at[rows], w2_out.at[rows], sems.at[len(copies)]))
            copies[-1].start()
    for pj in range(2):
        for y in range(size):
            for x in range(3):
                back = jnp.concatenate(
                    [tap(size - 1 - y, size - 1 - 2 * x + pj), tap(size - 1 - y, size - 2 - 2 * x + pj)], axis=1
                ).astype(BF16)
                for pi in range(2):
                    w = y + pi
                    lane = ((w // 2) * 3 + x) * 4 + (w % 2) * 2
                    row = (pi * 2 + pj) * ch1
                    w2b[row : row + ch1, lane * ch2 : (lane + 2) * ch2] = back
        for pi in range(2):
            rows = pl.ds((pi * 2 + pj) * ch1, ch1)
            copies.append(pltpu.make_async_copy(w2b.at[rows], w2b_out.at[rows], sems.at[len(copies)]))
            copies[-1].start()
    W = C + 2 * HJ
    lane = lax.broadcasted_iota(jnp.int32, (1, masks.shape[1]), 1)
    i = ((lane.astype(F32) + 0.5) * (1.0 / W)).astype(jnp.int32)
    j = lane - i * W - HJ
    frames = (
        (0, R, False), (0, R + 1, True), (-1, R + 1, True), (-3, R + 6, False), (-2, R + 4, False),
        (-1, R + 2, False), (-1, R + 2, True), (0, R, True), (0, R + 1, False), (-1, R + 1, False),
    )
    masks[...] = jnp.zeros(masks.shape, F32)
    for n, (start, count, mine) in enumerate(frames):
        r, c = i + start, j
        rows, columns = R, C
        if not mine:
            r, c = r + place[0] * R, c + place[1] * C
            rows, columns = R * high, C * across
        ok = (i < count) & (r >= 0) & (r < rows) & (c >= 0) & (c < columns)
        masks[n : n + 1, :] = jnp.where(ok, 1.0, 0.0)
    for copy in copies:
        copy.wait()


def cells_kernel(
    R, C, par, both, left, right, over, under, w1, b1, masks, pre, pool, msg_a, msg_b, sel, img, z, p1
):
    W = C + 2 * HJ
    G = W + 4
    frame = up128((R + 1) * W)
    px = W * S
    K = sel.shape[0]
    rows = R * S + 2 * RIM
    tile = 256
    for t in range(K // tile):
        p = lax.broadcasted_iota(jnp.int32, (K, tile), 0)
        n = lax.broadcasted_iota(jnp.int32, (K, tile), 1) + t * tile
        want = (p & (S - 1)) * G + (p >> 4)
        sel[:, t * tile : (t + 1) * tile] = jnp.where((n == want) & (p < px), 1.0, 0.0).astype(BF16)
    above, below = over[...].astype(F32), under[...].astype(F32)
    for f in range(2):
        for c in range(3):
            r = (f * 3 + c) * RIM
            mine = jnp.concatenate([v[f, c].astype(F32) for v in (left, both, right)], axis=1)
            whole = jnp.concatenate([above[r : r + RIM], mine, below[r : r + RIM]], axis=0)
            row = (f * 3 + c) * rows
            img[row : row + rows, :] = jnp.concatenate([whole, jnp.zeros((rows, K - px), F32)], axis=1)
    pixels = img[...].astype(BF16)
    for t in range(K // tile):
        lanes = slice(t * tile, (t + 1) * tile)
        z[:, lanes] = jnp.dot(pixels, sel[:, lanes], preferred_element_type=F32)
    own = masks[0:1, 0 : R * W]
    bias = wide(column(b1, 4), tile)
    for pi in range(2):
        top = 8 - 8 * pi
        for pj in range(2):
            for f in range(2):
                for s in range(S):
                    q = s + 8 * pj - 4
                    lane = (q % S) * G + q // S
                    parts = []
                    for k in range(R + 1):
                        r = top + S * k
                        parts.append(
                            jnp.concatenate(
                                [z[(f * 3 + c) * rows + r : (f * 3 + c) * rows + r + S, lane : lane + W] for c in range(3)],
                                axis=0,
                            )
                        )
                    parts.append(jnp.zeros((3 * S, frame - (R + 1) * W), F32))
                    p1[s * 48 : s * 48 + 48, f * frame : (f + 1) * frame] = jnp.concatenate(parts, axis=1).astype(BF16)
            for t in range(2 * frame // tile):
                lanes = slice(t * tile, (t + 1) * tile)
                pre[pi, pj, :, lanes] = jnp.dot(w1[...], p1[:, lanes], preferred_element_type=F32) + bias
            for f in range(2):
                v = pre[pi, pj, :, f * frame : (f + 1) * frame]
                feat = v * sigmoid(v)
                quarter = feat.shape[0] // 4
                mean = 0.25 * (
                    (feat[0:quarter] + feat[quarter : 2 * quarter])
                    + (feat[2 * quarter : 3 * quarter] + feat[3 * quarter :])
                )
                mine = mean[:, pi * W : pi * W + R * W]
                mine = jnp.where(own > 0.0, mine, 0.0)
                row = (f * 4 + pi * 2 + pj) * quarter
                even = lax.rem(par[0], 2) == 0
                head = lanes_of(mine, 0, 3 * W, msg_a.shape[1])
                tail = lanes_of(mine, (R - 3) * W, 3 * W, msg_a.shape[1])
                msg_a[row : row + quarter, :] = jnp.where(even, tail, head).astype(BF16)
                msg_b[row : row + quarter, :] = jnp.where(even, head, tail).astype(BF16)
                pool[row : row + quarter, :] = lanes_of(mine, 0, R * W, pool.shape[1]).astype(BF16)


def first_grad_kernel(pre, lin, masks, base, gain, loss):
    frame = base.shape[3]
    ch = lin.shape[1]
    total = jnp.zeros((1, frame), F32)
    weights = wide(column(lin), frame)
    for pi in range(2):
        for pj in range(2):
            for t in range(4):
                v0 = pre[pi, pj, t * ch : (t + 1) * ch, 0:frame]
                v1 = pre[pi, pj, t * ch : (t + 1) * ch, frame : 2 * frame]
                dfeat, slope, part = layer_terms(v0, v1, weights, 16.0)
                base[pi, pj, t * ch : (t + 1) * ch, :] = dfeat * slope
                gain[pi, pj, t * ch : (t + 1) * ch, :] = 0.25 * slope
                total = total + jnp.where(masks[1 + pi : 2 + pi, 0:frame] > 0.0, part, 0.0)
    loss[...] = jnp.broadcast_to(total, loss.shape)


def third_weights_kernel(order, place, b3, lin3, *refs):
    k3, (w3, w3b, consts, bias) = refs[: len(order)], refs[len(order) :]
    c2 = w3b.shape[0]
    c3 = w3.shape[0]
    shard = k3[0].shape[1]
    bias[0] = column(b3)
    bias[1] = column(lin3)
    for n, flip in enumerate(order):
        start = pl.multiple_of(jnp.bitwise_xor(place[2], flip) * shard, 8)
        for e in range(2):
            consts[e, n * shard : (n + 1) * shard, :] = bias[e, pl.ds(start, shard), :]
        for k in range(0, 9, 2):
            size = min(2, 9 - k) * c2
            taps = k3[n][k * c2 : k * c2 + size, :].astype(F32)
            w3[n * shard : (n + 1) * shard, k * c2 : k * c2 + size] = taps.T.astype(BF16)
    for k in range(9):
        taps = [k3[n][(8 - k) * c2 : (9 - k) * c2, :] for n in range(len(order))]
        w3b[:, k * c3 : (k + 1) * c3] = jnp.concatenate(taps, axis=1)


def middle_kernel(
    R, C, pixels, par, pool, rec_a, rec_b, masks, w2, b2, lin2, w3, consts, w3b, loss1, d2, msg_a, msg_b, loss,
    s1, p2, pre2, q2, s2, p3, pre3, s3, p3b,
):
    W = C + 2 * HJ
    even = lax.rem(par[0], 2) == 0
    n2 = up128((R + 4) * W)
    n3 = up128((R + 2) * W)
    n4 = up128(R * W)
    c1 = pool.shape[0] // 2
    c2 = b2.shape[1]
    c3 = w3.shape[0]
    ext = s1.shape[1]
    inside = masks[3:4, 0 : (R + 6) * W]
    for r in range(0, 2 * c1, 64):
        a = rec_a[r : r + 64, :].astype(F32)
        b = rec_b[r : r + 64, :].astype(F32)
        above = jnp.where(even, b, a)[:, 0 : 3 * W]
        below = jnp.where(even, a, b)[:, 0 : 3 * W]
        mine = pool[r : r + 64, :].astype(F32)[:, 0 : R * W]
        whole = jnp.concatenate([above, mine, below], axis=1)
        whole = jnp.where(inside > 0.0, whole, 0.0)
        s1[r : r + 64, :] = jnp.concatenate(
            [jnp.zeros((64, GUARD), F32), whole, jnp.zeros((64, ext - GUARD - (R + 6) * W), F32)], axis=1
        ).astype(BF16)
    for f in range(2):
        shift_all(p2, f * n2, s1, f * c1, c1, window(W, 3), n2)
    tile = 256
    bias2 = column(b2, 4)
    bias3 = consts[0]
    lins3 = consts[1]

    def second(t, carry):
        lanes = pl.ds(pl.multiple_of(t * tile, tile), tile)
        v = jnp.dot(w2[...], p2[:, lanes], preferred_element_type=F32) + wide(bias2, tile)
        pre2[:, lanes] = v
        feat = v * sigmoid(v)
        q2[:, lanes] = 0.25 * (
            (feat[0:c2] + feat[c2 : 2 * c2]) + (feat[2 * c2 : 3 * c2] + feat[3 * c2 :])
        )
        return carry

    lax.fori_loop(0, 2 * n2 // tile, second, 0)
    for f in range(2):
        good = jnp.where(masks[4:5, 0:n2] > 0.0, q2[:, f * n2 : (f + 1) * n2], 0.0)
        s2[f * c2 : (f + 1) * c2, 0:GUARD] = jnp.zeros((c2, GUARD), BF16)
        s2[f * c2 : (f + 1) * c2, GUARD : GUARD + n2] = good.astype(BF16)
        s2[f * c2 : (f + 1) * c2, GUARD + n2 :] = jnp.zeros((c2, s2.shape[1] - GUARD - n2), BF16)
        shift_all(p3, f * n3, s2, f * c2, c2, window(W, 3), n3)

    def third(t, carry):
        lanes = pl.ds(pl.multiple_of(t * tile, tile), tile)
        pre3[:, lanes] = jnp.dot(w3[...], p3[:, lanes], preferred_element_type=F32) + wide(bias3, tile)
        return carry

    lax.fori_loop(0, 2 * n3 // tile, third, 0)
    s3[:, 0:GUARD] = jnp.zeros((c3, GUARD), BF16)
    s3[:, GUARD + n3 :] = jnp.zeros((c3, s3.shape[1] - GUARD - n3), BF16)
    total = jnp.zeros((1, 128), F32)
    for t in range(n3 // 128):
        v0 = pre3[:, t * 128 : (t + 1) * 128]
        v1 = pre3[:, n3 + t * 128 : n3 + (t + 1) * 128]
        dfeat, slope, part = layer_terms(v0, v1, lins3, 256.0)
        lanes = slice(t * 128, (t + 1) * 128)
        d = jnp.where(masks[5:6, lanes] > 0.0, dfeat * slope, 0.0)
        s3[:, GUARD + t * 128 : GUARD + (t + 1) * 128] = d.astype(BF16)
        total = total + jnp.where(masks[6:7, lanes] > 0.0, part, 0.0)
    shift_all(p3b, 0, s3, 0, c3, window(W, 3), n4)
    up = 0.25 * jnp.dot(w3b[...], p3b[...], preferred_element_type=F32)
    total2 = jnp.zeros((1, n4), F32)
    weights = wide(column(lin2), n4)
    strips = []
    for t in range(4):
        rows = slice(t * c2, (t + 1) * c2)
        v0 = pre2[rows, 0:n2][:, 2 * W : 2 * W + n4]
        v1 = pre2[rows, n2 : 2 * n2][:, 2 * W : 2 * W + n4]
        dfeat, slope, part = layer_terms(v0, v1, weights, 64.0)
        d = jnp.where(masks[0:1, 0:n4] > 0.0, (dfeat + up) * slope, 0.0)
        d2[rows, :] = d.astype(BF16)
        total2 = total2 + jnp.where(masks[7:8, 0:n4] > 0.0, part, 0.0)
        strips.append(d)
    rest = jnp.zeros((c2, msg_a.shape[1] - 3 * W), F32)
    for pj in range(2):
        upper, lower = strips[pj], strips[2 + pj]
        head = jnp.concatenate([upper[:, 0:W], lower[:, 0:W], upper[:, W : 2 * W], rest], axis=1)
        tail = jnp.concatenate(
            [lower[:, (R - 2) * W : (R - 1) * W], upper[:, (R - 1) * W : R * W], lower[:, (R - 1) * W : R * W], rest],
            axis=1,
        )
        rows = slice(pj * c2, (pj + 1) * c2)
        msg_a[rows, :] = jnp.where(even, tail, head).astype(BF16)
        msg_b[rows, :] = jnp.where(even, head, tail).astype(BF16)
    each = (
        jnp.sum(loss1[0:1, :]) / (pixels // 16) + jnp.sum(total2) / (pixels // 64) + jnp.sum(total) / (pixels // 256)
    )
    loss[...] = jnp.full(loss.shape, each, F32)


def last_kernel(
    R, C, par, d2, rec_a, rec_b, masks, w2b_in, base_in, gain_in, w1b_in, out,
    s4, p2b, s5, p1b, g, sel, flat, w2b, base, gain, w1b, sems,
):
    pairs = ((w2b_in, w2b), (base_in, base), (gain_in, gain), (w1b_in, w1b))
    fetch = [pltpu.make_async_copy(a, b, sems.at[n]) for n, (a, b) in enumerate(pairs)]
    for copy in fetch:
        copy.start()
    W = C + 2 * HJ
    even = lax.rem(par[0], 2) == 0
    c2 = d2.shape[0]
    frame = base.shape[3]
    n4 = up128(R * W)
    ext = s4.shape[1]
    ch = w2b.shape[0] // 4
    inside = masks[4:5, 0 : (R + 4) * W]

    none = jnp.zeros((64, W), F32)
    for t in range(0, c2, 64):
        pi, row = t // (c2 // 2), t % (c2 // 2)
        a = rec_a[row : row + 64, :].astype(F32)
        b = rec_b[row : row + 64, :].astype(F32)
        above = jnp.where(even, b, a)
        below = jnp.where(even, a, b)
        strips = [[v[:, n * W : (n + 1) * W] for n in range(3)] for v in (above, below)]
        mine = d2[t : t + 64, :].astype(F32)[:, 0 : R * W]
        if pi == 0:
            parts = [none, strips[0][1], mine, strips[1][0], strips[1][2]]
        else:
            parts = [strips[0][0], strips[0][2], mine, strips[1][1], none]
        whole = jnp.where(inside > 0.0, jnp.concatenate(parts, axis=1), 0.0)
        s4[t : t + 64, :] = jnp.concatenate(
            [jnp.zeros((64, GUARD), F32), whole, jnp.zeros((64, ext - GUARD - (R + 4) * W), F32)], axis=1
        ).astype(BF16)
    shift_all(p2b, 0, s4, 0, c2, window(W, 4), frame)
    fetch[0].wait()
    for qi in range(2):
        around = p2b[(1 - qi) * 3 * c2 : (4 - qi) * 3 * c2, :]
        up = jnp.dot(w2b[qi * 2 * ch : (qi + 1) * 2 * ch, :], around, preferred_element_type=F32)
        good = masks[8 + qi : 9 + qi, 0:frame] > 0.0
        if qi == 0:
            fetch[1].wait()
            fetch[2].wait()
        for qj in range(2):
            part = up[qj * ch : (qj + 1) * ch]
            for t in range(4):
                rows = slice(t * ch, (t + 1) * ch)
                d = base[qi, qj, rows, :] + gain[qi, qj, rows, :] * part
                row = ((qi * 2 + qj) * 4 + t) * ch
                s5[row : row + ch, 0:GUARD] = jnp.zeros((ch, GUARD), BF16)
                s5[row : row + ch, GUARD : GUARD + frame] = jnp.where(good, d, 0.0).astype(BF16)
                s5[row : row + ch, GUARD + frame :] = jnp.zeros((ch, s5.shape[1] - GUARD - frame), BF16)
    fetch[3].wait()
    for qi in range(2):
        for qj in range(2):
            for wi in range(4):
                for wj in range(4):
                    y, x = 2 * qi + wi - 1, 2 * qj + wj - 1
                    dy, dx = y // 4, x // 4
                    y, x = y % 4, x % 4
                    row = (((y // 2) * 2 + x // 2) * 4 + (y % 2) * 2 + x % 2) * ch
                    off = GUARD + (dy + y // 2) * W + dx
                    p1b[(wi * 4 + wj) * ch : (wi * 4 + wj + 1) * ch, :] = s5[row : row + ch, :][
                        :, off : off + n4
                    ]
            g[qi, qj] = jnp.dot(w1b[...], p1b[...], preferred_element_type=F32)
    for s in range(0, S, 2):
        for c in range(3):
            for i in range(R):
                for qi in range(2):
                    parts = []
                    for e in range(2):
                        q = s + e
                        r = ((q % 8) * 3 + c) * 8
                        lane = i * W + HJ
                        parts.append(g[qi, q // 8, r : r + 8, lane : lane + C])
                    row = c * R * S + i * S + qi * 8
                    flat[row : row + 8, s * C : (s + 2) * C] = jnp.concatenate(parts, axis=1)
    K = S * C
    tile = 256
    for t in range(K // tile):
        p = lax.broadcasted_iota(jnp.int32, (tile, K), 0) + t * tile
        n = lax.broadcasted_iota(jnp.int32, (tile, K), 1)
        group = p // C
        sel[t * tile : (t + 1) * tile, :] = jnp.where(n == (p - group * C) * S + group, 1.0, 0.0).astype(BF16)
    v = flat[...]
    high = v.astype(BF16)
    low = (v - high.astype(F32)).astype(BF16)
    flat[...] = jnp.dot(high, sel[...], preferred_element_type=F32) + jnp.dot(
        low, sel[...], preferred_element_type=F32
    )
    for c in range(3):
        out[c] = flat[c * R * S : (c + 1) * R * S, :] / SPREADS[c]


def swap(a, b, axis):
    count = lax.axis_size(axis)
    first = lax.ppermute(a, axis, [(i, i ^ 1) for i in range(count)])
    second = [(i, (i + 1) % count) for i in range(1, count, 2)]
    second = second + [(j, i) for i, j in second]
    return first, lax.ppermute(b, axis, second)


def neighbours(head, tail, axis, where, count):
    even = where % 2 == 0
    a, b = swap(jnp.where(even, tail, head), jnp.where(even, head, tail), axis)
    zero = jnp.zeros_like(head)
    before = jnp.where(where > 0, jnp.where(even, b, a), zero)
    after = jnp.where(where < count - 1, jnp.where(even, a, b), zero)
    return before, after


class Far:
    def __init__(self, array):
        self.array = array


def call(kernel, outs, scratch, limit, work, *args, far=()):
    def place(a):
        if isinstance(a, Far):
            return pltpu.HBM
        return pltpu.SMEM if a.ndim == 1 else pltpu.VMEM

    specs = [pl.BlockSpec(memory_space=place(a)) for a in args]
    args = [a.array if isinstance(a, Far) else a for a in args]
    spaces = [pltpu.HBM if n in far else pltpu.VMEM for n in range(len(jax.tree.leaves(outs)))]
    out_specs = jax.tree.unflatten(jax.tree.structure(outs), [pl.BlockSpec(memory_space=m) for m in spaces])
    return pl.pallas_call(
        kernel,
        out_shape=outs,
        in_specs=specs,
        out_specs=out_specs,
        scratch_shapes=scratch,
        compiler_params=pltpu.CompilerParams(vmem_limit_bytes=limit * 2**20),
        cost_estimate=pl.CostEstimate(flops=int(work * 10**9), bytes_accessed=2**20, transcendentals=0),
    )(*args)


def local(
    image_gen, image_ref, kernel_one, bias_one, kernel_two, bias_two, kernel_three, bias_three,
    lin_first, lin_second, lin_third,
):
    R = image_gen.shape[1] // S
    C = image_gen.shape[2] // S
    W = C + 2 * HJ
    high = lax.axis_size("row") * lax.axis_size("chan")
    across = lax.axis_size("col")
    at_row = lax.axis_index("row") * lax.axis_size("chan") + lax.axis_index("chan")
    at_col = lax.axis_index("col")
    pixels = image_gen.shape[1] * image_gen.shape[2] * high * across
    ch1, ch2, ch3 = bias_one.shape[0], bias_two.shape[0], bias_three.shape[0]

    y, x, c, a, b = np.meshgrid(*(np.arange(n) for n in (3, 3, 3, 4, 4)), indexing="ij")
    want = jnp.asarray((x * 192 + b * 48 + c * 16 + y * 4 + a).reshape(1, -1), jnp.int32)
    place = jnp.stack([at_row, at_col, lax.axis_index("chan")]).astype(jnp.int32)
    shard = kernel_three.shape[3]

    def arr(shape, dtype=F32):
        return jax.ShapeDtypeStruct(shape, dtype)

    w1, w1b, w2, w2b, masks = call(
        functools.partial(weights_kernel, R, C, high, across),
        (
            arr((4 * ch1, 768), BF16),
            arr((192, 16 * ch1), BF16),
            arr((4 * ch2, 36 * ch1), BF16),
            arr((4 * ch1, 36 * ch2), BF16),
            arr((16, 1024)),
        ),
        [
            pltpu.VMEM((976, ch1), F32),
            pltpu.VMEM((4 * ch2, 36 * ch1), BF16),
            pltpu.VMEM((4 * ch1, 36 * ch2), BF16),
            pltpu.SemaphoreType.DMA((8,)),
        ],
        62, 5, place, want, kernel_one.reshape(-1, ch1), kernel_two, far=(2, 3),
    )
    offsets = jnp.array(OFFSETS, F32)[:, None, None]
    spreads = jnp.array(SPREADS, F32)[:, None, None]

    def normed(cut):
        return jnp.stack([((cut(image) - offsets) / spreads).astype(BF16) for image in (image_gen, image_ref)])

    edge = HJ * S
    left, right = neighbours(
        normed(lambda image: image[:, :, :edge]), normed(lambda image: image[:, :, -edge:]), "col", at_col, across
    )
    both = normed(lambda image: image)

    def strip(rows):
        whole = jnp.concatenate([left[:, :, rows], both[:, :, rows], right[:, :, rows]], axis=3)
        return whole.reshape(6 * RIM, W * S)

    over, under = neighbours(strip(slice(0, RIM)), strip(slice(-RIM, None)), ROWS, at_row, high)
    span = (W + 4) * S
    over, under, kernel_three, w1, masks = lax.optimization_barrier((over, under, kernel_three, w1, masks))
    parts = lax.axis_size("chan")

    def widen(pieces, order, step):
        pairs = [(i, i ^ step) for i in range(parts)]
        pieces = pieces + [lax.ppermute(piece, "chan", pairs) for piece in pieces]
        return pieces, order + [n ^ step for n in order]

    pieces, order, step = [kernel_three.reshape(-1, shard)], [0], parts // 2
    if step > 0:
        pieces, order = widen(pieces, order, step)

    def flat(values):
        return values.reshape(1, -1)

    b1, b2, b3 = flat(bias_one), flat(bias_two), flat(bias_three)
    lin1, lin2, lin3 = flat(lin_first), flat(lin_second), flat(lin_third)

    frame = up128((R + 1) * W)
    n2, n3, n4 = up128((R + 4) * W), up128((R + 2) * W), up128(R * W)
    rows = 3 * (R * S + 2 * RIM)

    pre, pool, msg_a, msg_b = call(
        functools.partial(cells_kernel, R, C),
        (
            arr((2, 2, 4 * ch1, 2 * frame)),
            arr((8 * ch1, n4), BF16),
            arr((8 * ch1, up128(3 * W)), BF16),
            arr((8 * ch1, up128(3 * W)), BF16),
        ),
        [pltpu.VMEM((span, span), BF16), pltpu.VMEM((2 * rows, span), F32), pltpu.VMEM((2 * rows, span), F32),
         pltpu.VMEM((768, 2 * frame), BF16)],
        24, 5, place, both, left, right, over, under, w1, b1, masks,
    )
    rec_a, rec_b = swap(msg_a, msg_b, ROWS)
    base, gain, loss1 = call(
        first_grad_kernel,
        (arr((2, 2, 4 * ch1, frame)), arr((2, 2, 4 * ch1, frame)), arr((8, frame))),
        [],
        12, 3, pre, lin1, masks,
    )
    loss1, pieces = lax.optimization_barrier((loss1, pieces))
    while step > 1:
        step //= 2
        pieces, order = widen(pieces, order, step)
    w3, w3b, consts = call(
        functools.partial(third_weights_kernel, tuple(order)),
        (arr((ch3, 9 * ch2), BF16), arr((ch2, 9 * ch3), BF16), arr((2, ch3, 128))),
        [pltpu.VMEM((2, ch3, 128), F32)],
        12, 2, place, b3, lin3, *pieces,
    )
    ext1 = GUARD + up128((R + 6) * W) + GUARD
    everyone = high * across
    d2, msg_a, msg_b, each = call(
        functools.partial(middle_kernel, R, C, pixels),
        (
            arr((4 * ch2, n4), BF16),
            arr((2 * ch2, up128(3 * W)), BF16),
            arr((2 * ch2, up128(3 * W)), BF16),
            arr((everyone, 8, 128)),
        ),
        [
            pltpu.VMEM((8 * ch1, ext1), BF16),
            pltpu.VMEM((36 * ch1, 2 * n2), BF16),
            pltpu.VMEM((4 * ch2, 2 * n2), F32),
            pltpu.VMEM((ch2, 2 * n2), F32),
            pltpu.VMEM((2 * ch2, GUARD + n2 + GUARD), BF16),
            pltpu.VMEM((9 * ch2, 2 * n3), BF16),
            pltpu.VMEM((ch3, 2 * n3), F32),
            pltpu.VMEM((ch3, GUARD + n3 + GUARD), BF16),
            pltpu.VMEM((9 * ch3, n4), BF16),
        ],
        30, 10, place, pool, rec_a, rec_b, masks, w2, b2, lin2, w3, consts, w3b, loss1,
    )
    rec_a, rec_b = swap(msg_a, msg_b, ROWS)
    everywhere = lax.all_to_all(each, ("row", "col", "chan"), 0, 0)
    image_grad = call(
        functools.partial(last_kernel, R, C),
        arr(image_gen.shape),
        [
            pltpu.VMEM((4 * ch2, GUARD + up128((R + 4) * W) + GUARD), BF16),
            pltpu.VMEM((48 * ch2, frame), BF16),
            pltpu.VMEM((16 * ch1, GUARD + frame + GUARD), BF16),
            pltpu.VMEM((16 * ch1, n4), BF16),
            pltpu.VMEM((2, 2, 192, n4), F32),
            pltpu.VMEM((S * C, S * C), BF16),
            pltpu.VMEM((3 * R * S, S * C), F32),
            pltpu.VMEM(w2b.shape, BF16),
            pltpu.VMEM(base.shape, F32),
            pltpu.VMEM(gain.shape, F32),
            pltpu.VMEM(w1b.shape, BF16),
            pltpu.SemaphoreType.DMA((4,)),
        ],
        62, 10, place, d2, rec_a, rec_b, masks, Far(w2b), Far(base), Far(gain), Far(w1b),
    )
    everywhere, image_grad = lax.optimization_barrier((everywhere, image_grad))
    return image_grad, jnp.sum(everywhere[:, 0, 0])


def solution(mesh):
    tile = P(None, ROWS, "col")
    return jax.shard_map(
        local,
        mesh=mesh,
        in_specs=(tile, tile, P(), P(), P(), P(), P(None, None, None, "chan"), P(), P(), P(), P()),
        out_specs=(tile, P()),
        check_vma=False,
    )
```
